256 devices in a mesh: patch: 64 (over z, x, core), pair: 4 (over y).
Axes of the slice: x: 4, y: 4, z: 8, core: 2. Of those that a mesh axis runs over, the one named last changes fastest.
Arguments:
- node_latents: bfloat16 [65536, 1024], P('patch', 'pair'), may hold values from -12 to 12
- edge_latents: bfloat16 [131072, 1024], P('patch', 'pair'), may hold values from -12 to 12
- edge_sender: int32 [512, 256], P('patch'), may hold values from -1 to 2047, as said below
- edge_receiver: int32 [512, 256], P('patch'), may hold values from -1 to 31, as said below
- block_owner: int32 [512], P('patch'), may hold values from 0 to 63, as said below
- node_counts: int32 [64], P('patch'), may hold values from 512 to 1024, as said below
- halo_nodes: int32 [64, 64, 32], P('patch'), may hold values from 0 to 1023, as said below
- w_endpoints: bfloat16 [1024, 2, 1024], P(None, None, 'pair'), may hold values from -0.1875 to 0.1875
- w_edge_in: bfloat16 [1024, 1024], P(None, 'pair'), may hold values from -0.1875 to 0.1875
- edge_bias: float32 [1024], P('pair'), may hold values from -3 to 3
- w_edge_out: bfloat16 [1024, 1024], P('pair'), may hold values from -1 to 1
- edge_gain: float32 [1024], P('pair'), may hold values from 0.5 to 1.5
- edge_shift: float32 [1024], P('pair'), may hold values from -3 to 3
- w_node_in: bfloat16 [2, 1024, 1024], P(None, None, 'pair'), may hold values from -0.125 to 0.125
- node_bias: float32 [1024], P('pair'), may hold values from -3 to 3
- w_node_out: bfloat16 [1024, 1024], P('pair'), may hold values from -1 to 1
- node_gain: float32 [1024], P('pair'), may hold values from 0.5 to 1.5
- node_shift: float32 [1024], P('pair'), may hold values from -3 to 3
Outputs:
- updated_nodes: bfloat16 [65536, 1024], P('patch', 'pair')
- updated_edges: bfloat16 [131072, 1024], P('patch', 'pair')
The draws below stay inside these ranges and needn't reach their ends.
Inputs may be any that keep to these rules, and one draw needn't show every extreme that they name: `edge_sender`: section q = slot // 32 of a patch's halo table holds, in order, the nodes halo_nodes[q, that patch]; -1 stands exactly where edge_receiver is -1. `edge_receiver`: -1 marks padding and stands only after the live edges of a block; within a block the live values never fall and take at most 16 distinct values; every patch has a block with 256 live edges and 16 distinct receivers. `block_owner`: no patch owns more than 1 of the blocks of one patch; every patch owns 1 of its own blocks, and some patch owns 1 block of every patch. `node_counts`: some patch has 1024 live nodes. halo_nodes[q, d] lists local live nodes of patch q (below node_counts[q]); entries may repeat.
All inputs are finite; a program needn't handle non-finite values.
Results may differ from the reference program's by a relative error of at most 0.008.
Values may be sent and summed in bfloat16 or wider, within the bound.
A program may use at most 128 MiB of HBM per device.

```python
import math
import jax
import jax.numpy as jnp
from jax import lax

D = 1024
TILE = 256
RT = 16
NODE_DEV = 1024
BLK_DEV = 8
CAP = 1
HALO = 32
HOT = 4
BLOCKS = 512
EDGES = 131072
NODES = 65536
N_PATCH = 64
N_PAIR = 4


def layout_ints(key):
    keys = jax.random.split(jax.random.fold_in(key, 101), 12)
    patch_ids = jnp.arange(N_PATCH, dtype=jnp.int32)
    hot_order = jnp.argsort(jax.random.randint(keys[0], (N_PATCH,), 0, 2 ** 20, dtype=jnp.int32) * N_PATCH + patch_ids)
    hot_rank = jnp.zeros((N_PATCH,), jnp.int32).at[hot_order].set(patch_ids)
    is_hot = (hot_rank < HOT).astype(jnp.int32)
    scores = jax.random.randint(keys[1], (N_PATCH, N_PATCH), 0, 2 ** 20, dtype=jnp.int32)
    scores = scores + is_hot[None, :] * 2 ** 21 + (patch_ids[:, None] == patch_ids[None, :]).astype(jnp.int32) * 2 ** 22
    scores = scores * N_PATCH + patch_ids[None, :]
    chosen = lax.top_k(scores, BLK_DEV // CAP)[1].astype(jnp.int32)
    chosen = jnp.repeat(chosen, CAP, axis=1)
    shuffle_score = jax.random.randint(keys[2], (N_PATCH, BLK_DEV), 0, 2 ** 20, dtype=jnp.int32) * BLK_DEV + jnp.arange(BLK_DEV, dtype=jnp.int32)[None, :]
    order = jnp.argsort(shuffle_score, axis=1)
    owners = jnp.take_along_axis(chosen, order, axis=1).reshape(BLOCKS).astype(jnp.int32)
    counts = jax.random.randint(keys[3], (N_PATCH,), NODE_DEV // 2, NODE_DEV + 1, dtype=jnp.int32)
    counts = jnp.where(is_hot > 0, NODE_DEV, counts).astype(jnp.int32)
    halo_lists = jax.random.randint(keys[4], (N_PATCH, N_PATCH, HALO), 0, counts[:, None, None], dtype=jnp.int32)
    block_ids = jnp.arange(BLOCKS, dtype=jnp.int32)
    live_count = jax.random.randint(keys[5], (BLOCKS,), TILE // 2, TILE + 1, dtype=jnp.int32)
    full_pick = jax.random.randint(keys[6], (N_PATCH,), 0, BLK_DEV, dtype=jnp.int32)
    live_count = jnp.where(block_ids % BLK_DEV == jnp.repeat(full_pick, BLK_DEV), TILE, live_count)
    fillers = jax.random.randint(keys[7], (BLOCKS, TILE - RT), 0, RT, dtype=jnp.int32)
    firsts = jnp.broadcast_to(jnp.arange(RT, dtype=jnp.int32)[None, :], (BLOCKS, RT))
    segment = jnp.sort(jnp.concatenate([firsts, fillers], axis=1), axis=1)
    slot_score = jax.random.randint(keys[8], (BLOCKS, HALO), 0, 2 ** 20, dtype=jnp.int32) * HALO + jnp.arange(HALO, dtype=jnp.int32)[None, :]
    slot_list = jnp.sort(jnp.argsort(slot_score, axis=1)[:, :RT].astype(jnp.int32), axis=1)
    positions = jnp.arange(TILE, dtype=jnp.int32)[None, :]
    is_live = positions < live_count[:, None]
    receiver = jnp.where(is_live, jnp.take_along_axis(slot_list, segment, axis=1), -1).astype(jnp.int32)
    coin = jax.random.randint(keys[9], (BLOCKS, TILE), 0, 2, dtype=jnp.int32)
    other = jax.random.randint(keys[10], (BLOCKS, TILE), 0, N_PATCH, dtype=jnp.int32)
    section = jnp.where(coin > 0, owners[:, None], other)
    within = jax.random.randint(keys[11], (BLOCKS, TILE), 0, HALO, dtype=jnp.int32)
    sender = jnp.where(is_live, section * HALO + within, -1).astype(jnp.int32)
    return (owners, counts, halo_lists, sender, receiver)


def draw_edge_sender(key, part):
    return layout_ints(key)[3]


def draw_edge_receiver(key, part):
    return layout_ints(key)[4]


def draw_block_owner(key, part):
    return layout_ints(key)[0]


def draw_node_counts(key, part):
    return layout_ints(key)[1]


def draw_halo_nodes(key, part):
    return layout_ints(key)[2]


def scaled_rows(key, rows_count, cols_count):
    key_base, key_scale = jax.random.split(jax.random.fold_in(key, 5), 2)
    base = jax.random.normal(key_base, (rows_count, cols_count), jnp.float32)
    scale = jnp.exp(jax.random.uniform(key_scale, (rows_count, 1), jnp.float32, math.log(0.3), math.log(3.0)))
    value = base * scale
    return jnp.clip(value, -12.0, 12.0)


def draw_node_latents(key, part):
    return scaled_rows(key, NODES, D).astype(jnp.bfloat16)


def draw_edge_latents(key, part):
    return scaled_rows(key, EDGES, D).astype(jnp.bfloat16)


def rising_columns(key):
    key_base, key_jitter = jax.random.split(jax.random.fold_in(key, 9), 2)
    base = jax.random.normal(key_base, (D, D), jnp.float32) / math.sqrt(D)
    ramp = (jnp.arange(D, dtype=jnp.float32) / (D - 1))[None, :]
    scale = jnp.exp(math.log(0.5) + ramp * math.log(10.0)) * jax.random.uniform(key_jitter, (1, D), jnp.float32, 0.7, 1.3)
    return jnp.clip(base * scale, -1.0, 1.0).astype(jnp.bfloat16)


def draw_w_edge_out(key, part):
    return rising_columns(key)


def draw_w_node_out(key, part):
    return rising_columns(jax.random.fold_in(key, 3))


def block_scale(rng, extent, pieces, low, high):
    level = 1.0
    for axis_at, parts in pieces:
        draws = jax.random.uniform(jax.random.fold_in(jax.random.fold_in(rng, 6), axis_at), (parts,), jnp.float32, low / len(pieces), high / len(pieces))
        level = level * jnp.repeat(jnp.exp(draws), extent[axis_at] // parts).reshape((-1,) + (1,) * (len(extent) - 1 - axis_at))
    return level


def scatter_about(rng, dims, deviation, reach, cuts=(), kind=jnp.bfloat16):
    values = deviation * jax.random.normal(rng, dims, jnp.float32)
    if cuts:
        values = values * block_scale(rng, dims, cuts, -0.22, 0.18)
    return jnp.clip(values, -reach, reach).astype(kind)


def setup_inputs(seed: int = 0) -> dict:
    key_of = jax.random.split(jax.random.key(seed), 19)
    return {
        "node_latents": draw_node_latents(jax.random.fold_in(key_of[18], 71), 0),
        "edge_latents": draw_edge_latents(jax.random.fold_in(key_of[18], 71), 0),
        "edge_sender": draw_edge_sender(jax.random.fold_in(key_of[18], 71), 0),
        "edge_receiver": draw_edge_receiver(jax.random.fold_in(key_of[18], 71), 0),
        "block_owner": draw_block_owner(jax.random.fold_in(key_of[18], 71), 0),
        "node_counts": draw_node_counts(jax.random.fold_in(key_of[18], 71), 0),
        "halo_nodes": draw_halo_nodes(jax.random.fold_in(key_of[18], 71), 0),
        "w_endpoints": scatter_about(key_of[7], (D, 2, D), D ** -0.5, 0.1875, ((2, 4),)),
        "w_edge_in": scatter_about(key_of[8], (D, D), D ** -0.5, 0.1875, ((1, 4),)),
        "edge_bias": scatter_about(key_of[9], (D,), 0.5, 3.0, ((0, 4),), jnp.float32),
        "w_edge_out": draw_w_edge_out(jax.random.fold_in(key_of[18], 71), 0),
        "edge_gain": jnp.clip(1.0 + 0.1 * jax.random.normal(key_of[11], (D,), jnp.float32), 0.5, 1.5),
        "edge_shift": scatter_about(key_of[12], (D,), 0.5, 3.0, ((0, 4),), jnp.float32),
        "w_node_in": scatter_about(key_of[13], (2, D, D), (2 * D) ** -0.5, 0.125, ((2, 4),)),
        "node_bias": scatter_about(key_of[14], (D,), 0.5, 3.0, ((0, 4),), jnp.float32),
        "w_node_out": draw_w_node_out(jax.random.fold_in(key_of[18], 71), 0),
        "node_gain": jnp.clip(1.0 + 0.1 * jax.random.normal(key_of[16], (D,), jnp.float32), 0.5, 1.5),
        "node_shift": scatter_about(key_of[17], (D,), 0.5, 3.0, ((0, 4),), jnp.float32),
    }


EPS = 1e-05

def pair_sum(hidden, weight):
    rows_count = hidden.shape[0]
    share = weight.shape[0] // N_PAIR
    total_sum = jnp.zeros((rows_count, weight.shape[1]), jnp.float32)
    for member in range(N_PAIR):
        term = jnp.dot(hidden[:, member * share:(member + 1) * share], weight[member * share:(member + 1) * share], preferred_element_type=jnp.float32)
        rounded = lax.optimization_barrier(term.astype(jnp.bfloat16))
        total_sum = total_sum + rounded.astype(jnp.float32)
    return total_sum

def normalize(values, gain_row, shift_row):
    row_mean = lax.optimization_barrier(jnp.mean(values, axis=1, keepdims=True))
    square = lax.optimization_barrier(jnp.mean(values * values, axis=1, keepdims=True))
    return (values - row_mean) * lax.rsqrt(square - row_mean * row_mean + EPS) * gain_row[None, :] + shift_row[None, :]

def reference(node_latents, edge_latents, edge_sender, edge_receiver, block_owner, node_counts, halo_nodes, w_endpoints, w_edge_in, edge_bias, w_edge_out, edge_gain, edge_shift, w_node_in, node_bias, w_node_out, node_gain, node_shift):
    projected = jnp.dot(node_latents, w_endpoints.reshape(D, 2 * D), preferred_element_type=jnp.float32).astype(jnp.bfloat16).reshape(NODES, 2, D)
    device_edges = BLK_DEV * TILE

    def one_device(aggregate, device):
        rows_in = lax.dynamic_slice_in_dim(edge_latents, (device * device_edges).astype(jnp.int32), device_edges, 0)
        senders = lax.dynamic_slice_in_dim(edge_sender, (device * BLK_DEV).astype(jnp.int32), BLK_DEV, 0).reshape(-1)
        receivers = lax.dynamic_slice_in_dim(edge_receiver, (device * BLK_DEV).astype(jnp.int32), BLK_DEV, 0).reshape(-1)
        owners = lax.dynamic_slice_in_dim(block_owner, (device * BLK_DEV).astype(jnp.int32), BLK_DEV, 0)
        edge_owner = jnp.repeat(owners, TILE)
        is_live = receivers >= 0
        sender_clip = jnp.maximum(senders, 0)
        sender_patch = sender_clip // HALO
        sender_node = sender_patch * NODE_DEV + halo_nodes[sender_patch, device, sender_clip - sender_patch * HALO]
        receiver_node = edge_owner * NODE_DEV + halo_nodes[edge_owner, device, jnp.maximum(receivers, 0)]
        edge_pre = jnp.dot(rows_in, w_edge_in, preferred_element_type=jnp.float32)
        edge_pre = edge_pre + projected[sender_node, 0].astype(jnp.float32) + projected[receiver_node, 1].astype(jnp.float32) + edge_bias[None, :]
        edge_hidden = jax.nn.silu(edge_pre).astype(jnp.bfloat16)
        edge_mixed = pair_sum(edge_hidden, w_edge_out)
        edge_norm = normalize(edge_mixed, edge_gain, edge_shift)
        old_rows = rows_in.astype(jnp.float32)
        new_rows = jnp.where(is_live[:, None], old_rows + edge_norm, old_rows).astype(jnp.bfloat16)
        target = jnp.where(is_live, receiver_node, NODES).astype(jnp.int32)
        aggregate = aggregate.at[target].add(new_rows.astype(jnp.float32))
        return (aggregate, new_rows)
    aggregate, new_edges = lax.scan(one_device, jnp.zeros((NODES + 1, D), jnp.float32), jnp.arange(N_PATCH, dtype=jnp.int32))
    aggregated = aggregate[:NODES].astype(jnp.bfloat16)
    node_pre = jnp.dot(node_latents, w_node_in[0], preferred_element_type=jnp.float32)
    node_pre = node_pre + jnp.dot(aggregated, w_node_in[1], preferred_element_type=jnp.float32) + node_bias[None, :]
    node_hidden = jax.nn.silu(node_pre).astype(jnp.bfloat16)
    node_mixed = pair_sum(node_hidden, w_node_out)
    node_norm = normalize(node_mixed, node_gain, node_shift)
    live_nodes = jnp.arange(NODES, dtype=jnp.int32) % NODE_DEV < jnp.repeat(node_counts, NODE_DEV)
    old_nodes = node_latents.astype(jnp.float32)
    updated_nodes = jnp.where(live_nodes[:, None], old_nodes + node_norm, old_nodes).astype(jnp.bfloat16)
    return (updated_nodes, new_edges.reshape(EDGES, D))
```

```python
import jax
import jax.numpy as jnp
from jax import lax
from jax.experimental import pallas as pl
from jax.experimental.pallas import tpu as pltpu
from jax.sharding import PartitionSpec as P

EPS = 1e-05
MESH = pl.DeviceIdType.MESH
BF = jnp.bfloat16
F32 = jnp.float32
I32 = jnp.int32

NODE = 1024
EDGE = 2048
FEAT = 256
WIDE = 1024
PATCH = 64
HALO = 32
RT = 16
BLK = 8
TILE = 256
ROWS = 2 * TILE
SEL = ROWS + 2 * HALO
NROW = NODE // 4
ANY = pl.BlockSpec(memory_space=pl.ANY)
VM = pl.BlockSpec(memory_space=pltpu.VMEM)
SM = pl.BlockSpec(memory_space=pltpu.SMEM)


def iota(shape, dim):
    return lax.broadcasted_iota(I32, shape, dim)


def hot(mask):
    return jnp.where(mask, 1.0, 0.0).astype(BF)


def dot(a, b):
    return jnp.dot(a, b, preferred_element_type=F32)


def silu(v):
    return v / (1.0 + jnp.exp(-v))


def aligned(v, n):
    return pl.multiple_of(v, n)


def kernel(
    nl, el, snd, rcv, own, cnt, hal, wep, win, eb, wout, eg, es, wnin, nb, wnout, ng, ns,
    o_n, o_e,
    nl_v, pcol, picked, halo_r, idcol, rcol, idt, rank8, idr, vec, gacc, sbuf, xs,
    xe, xn, wa, wb, acc, hid, outb, tsb, tsr, sv, vv, amat, abuf, xa, acc2, outn,
    loc, hs, hr, ids_s, ids_r, es_, er_, xns, xnr, vs, vr,
    wys, wyr, wxs, wxr, wds, wdr, ss, sr, tss, tsrr, v2s, v2r, as_, ar_, oes, oer, ons, onr,
):
    me = lax.axis_index("patch")
    j = lax.axis_index("pair")
    z, x, c = me // 8, lax.rem(me // 2, 4), lax.rem(me, 2)

    def dz_of(m):
        odd = lax.rem(m, 2)
        return lax.rem(odd * ((m + 1) // 2) + (1 - odd) * (8 - m // 2), 8)

    def place(m, t):
        return lax.rem(x + t // 2, 4) * 2 + lax.rem(c + lax.rem(t, 2), 2)

    def dest(m, t):
        return lax.rem(z + dz_of(m), 8) * 8 + place(m, t)

    def rem(src, dst, s, r, dev):
        return pltpu.make_async_remote_copy(
            src_ref=src, dst_ref=dst, send_sem=s, recv_sem=r, device_id=dev, device_id_type=MESH
        )

    def pair_of(dy):
        return lax.rem(j + dy, 4)

    loads = []

    def load(src, dst):
        copy = pltpu.make_async_copy(src, dst, loc.at[len(loads)])
        copy.start()
        loads.append(copy)
        return copy

    ld_nl = load(nl, nl_v)
    ld_e = [load(win, wa.at[0, 0]), load(wep.at[0], wa.at[0, 1]), load(wep.at[1], wa.at[0, 2])]
    ld_e.append(load(wout, wb.at[0, 0]))
    my_cols = pl.ds(aligned(j * FEAT, FEAT), FEAT)
    my_edges = pl.ds(aligned(j * ROWS, ROWS), ROWS)
    my_nodes = pl.ds(aligned(j * NROW, NROW), NROW)
    ld_x = [load(el.at[my_edges], xe.at[:, my_cols]), load(nl.at[my_nodes], xn.at[:, my_cols])]
    ld_n = [load(wnin.at[0], wa.at[0, 3]), load(wnin.at[1], wa.at[0, 4]), load(wnout, wb.at[0, 1])]

    barrier = pltpu.get_barrier_semaphore()

    def greet(r, carry):
        pl.semaphore_signal(
            barrier, inc=1, device_id=(dest(r // 8, lax.rem(r, 8)), j), device_id_type=MESH
        )
        return carry

    lax.fori_loop(1, PATCH, greet, 0)
    for dy in (1, 2, 3):
        pl.semaphore_signal(barrier, inc=1, device_id=(me, pair_of(dy)), device_id_type=MESH)

    hal_t = jnp.concatenate([hal[0], jnp.zeros((PATCH, 128 - HALO), I32)], axis=1).T
    for d in range(PATCH):
        pcol[d * HALO : (d + 1) * HALO, :] = hal_t[0:HALO, d : d + 1]
    ld_nl.wait()

    def pick(m):
        base = aligned(lax.rem(z + dz_of(m), 8) * 256, 256)
        ones = hot(pcol[pl.ds(base, 256), :] == iota((256, NODE), 1))
        picked[pl.ds(aligned(m * 256, 256), 256), :] = dot(ones, nl_v[...]).astype(BF)

    def halo_copy(m, t):
        return rem(
            picked.at[pl.ds(aligned(m * 256 + place(m, t) * HALO, HALO), HALO)],
            halo_r.at[pl.ds(aligned((m * 8 + t) * HALO, HALO), HALO)],
            hs,
            hr.at[m // 2],
            (dest(m, t), j),
        )

    pick(0)
    pl.semaphore_wait(barrier, PATCH - 1 + 3)

    row_a = pl.ds(aligned((c * 4 + x) * 128, 128), 128)
    row_b = pl.ds(aligned((c * 4 + x) * 32, 32), 32)
    units = ((0, 3, 0), (3, 2, 1))

    def weights_y(k):
        first, count, b = units[k]
        copies = []
        for dy in (2, 1, 3):
            dev = (me, pair_of(dy))
            i = dy - 1
            copies.append(rem(
                wa.at[0, pl.ds(first, count), row_a], wa.at[4 - dy, pl.ds(first, count), row_a],
                wys.at[2 * k, i], wyr.at[2 * k, i], dev,
            ))
            copies.append(rem(
                wb.at[0, b, row_b], wb.at[4 - dy, b, row_b],
                wys.at[2 * k + 1, i], wyr.at[2 * k + 1, i], dev,
            ))
        return copies

    def weights_x(k):
        first, count, b = units[k]
        copies = []
        for dx in (2, 1, 3):
            dev = (z * 8 + lax.rem(x + dx, 4) * 2 + c, j)
            i = dx - 1
            part = wa.at[pl.ds(1, 3), pl.ds(first, count), row_a]
            copies.append(rem(part, part, wxs.at[2 * k, i], wxr.at[2 * k, i], dev))
            part = wb.at[pl.ds(1, 3), b, row_b]
            copies.append(rem(part, part, wxs.at[2 * k + 1, i], wxr.at[2 * k + 1, i], dev))
        return copies

    def weights_d(k):
        first, count, b = units[k]
        dev = (z * 8 + x * 2 + 1 - c, j)
        part = wa.at[pl.ds(1, 3), pl.ds(first, count), pl.ds(aligned(c * 512, 512), 512)]
        other = wb.at[pl.ds(1, 3), b, pl.ds(aligned(c * 128, 128), 128)]
        return [
            rem(part, part, wds.at[2 * k], wdr.at[2 * k], dev),
            rem(other, other, wds.at[2 * k + 1], wdr.at[2 * k + 1], dev),
        ]

    sent = []

    def start(copies):
        for copy in copies:
            copy.start()
        sent.extend(copies)
        return copies

    def landed(copies):
        for copy in copies:
            copy.wait_recv()

    def send_plane(m, first):
        def step(t, carry):
            halo_copy(m, t).start()
            return carry

        lax.fori_loop(first, 8, step, 0)

    send_plane(0, 1)
    for copy in ld_e:
        copy.wait()
    ey = start(weights_y(0))

    def plane(m, carry):
        pick(m)
        send_plane(m, 0)
        return carry

    lax.fori_loop(1, 8, plane, 0)
    halo_r[0:HALO, :] = picked[pl.ds(aligned((x * 2 + c) * HALO, HALO), HALO), :]

    edges_in = start([
        rem(
            el.at[pl.ds(aligned(pair_of(dy) * ROWS, ROWS), ROWS)], xe.at[:, my_cols],
            es_.at[dy - 1], er_.at[dy - 1], (me, pair_of(dy)),
        )
        for dy in (2, 1, 3)
    ])
    for i, ref in enumerate((eb, eg, es, nb, ng, ns)):
        vec[j, i : i + 1, :] = ref[...]

    vecs = start([
        rem(vec.at[j], vec.at[j], vs.at[dy - 1], vr.at[dy - 1], (me, pair_of(dy)))
        for dy in (2, 1, 3)
    ])

    snd_t = snd[...].T
    rcv_t = rcv[...].T
    lane = iota((TILE, 128), 1)
    for b in range(BLK):
        half = (b % 2) * TILE
        idcol[b // 2, half : half + TILE, :] = snd_t[:, b : b + 1]
        low = ROWS + (b % 2) * HALO
        idcol[b // 2, low : low + HALO, :] = iota((HALO, 1), 0) + own[b] * HALO
        rcol[b] = rcv_t[:, b : b + 1]
        seen = jnp.max(jnp.where(rcv_t[:, b : b + 1] == lane, 1, 0), axis=0, keepdims=True)
        idt[b : b + 1, :] = jnp.where(iota((1, 128), 1) == HALO, own[b], seen)
    low_tri = hot(iota((128, 128), 0) < iota((128, 128), 1))
    live8 = jnp.where(iota((BLK, 128), 1) < HALO, idt[...], 0)
    rank8[...] = jnp.where(live8 > 0, dot(live8.astype(F32).astype(BF), low_tri), -1.0)

    def ids_copy(r):
        return rem(idt, idr.at[me], ids_s, ids_r, (dest(r // 8, lax.rem(r, 8)), j))

    def ids_step(r, carry):
        ids_copy(r).start()
        return carry

    lax.fori_loop(1, PATCH, ids_step, 0)
    idr[me] = idt[...]

    def gather(g):
        slot = g * 16 + iota((1, 512), 1) // HALO
        m = slot // 8
        odd = lax.rem(m, 2)
        dz = odd * ((m + 1) // 2) + (1 - odd) * (8 - m // 2)
        t = lax.rem(slot, 8)
        source = (
            lax.rem(z - dz + 16, 8) * 8 + lax.rem(x - t // 2 + 4, 4) * 2
            + lax.rem(c + lax.rem(t, 2), 2)
        )
        ident = source * HALO + lax.rem(iota((1, 512), 1), HALO)
        low = HALO if g == 0 else 0
        count = 512 - low
        arrived = halo_r.at[pl.ds(g * 512 + low, count)]
        pltpu.make_async_copy(arrived, arrived, hr.at[g]).wait()
        for dy in (2, 1, 3, 0):
            ones = hot(idcol[pair_of(dy)] == ident)
            part = dot(ones, halo_r[g * 512 : (g + 1) * 512, :])
            if g == 0:
                gacc[dy] = part
            elif g < 3:
                gacc[dy] += part
            elif dy == 0:
                xs[:, my_cols] = (gacc[dy] + part).astype(BF)
            else:
                sbuf[dy - 1] = (gacc[dy] + part).astype(BF)
                start([rem(
                    sbuf.at[dy - 1], xs.at[:, my_cols], ss.at[dy - 1], sr.at[dy - 1],
                    (me, pair_of(dy)),
                )])

    gather(0)
    gather(1)
    landed(ey)
    ex = start(weights_x(0))
    gather(2)
    mark = len(sent)
    gather(3)
    rows_in = sent[mark:]

    for copy in ld_x + ld_n:
        copy.wait()
    nodes_in = start([
        rem(
            nl.at[pl.ds(aligned(pair_of(dy) * NROW, NROW), NROW)], xn.at[:, my_cols],
            xns.at[dy - 1], xnr.at[dy - 1], (me, pair_of(dy)),
        )
        for dy in (2, 1, 3)
    ])
    landed(ex)
    ed = start(weights_d(0))

    all_ids = pltpu.make_async_copy(idr.at[pl.ds(0, 63)], idr.at[pl.ds(0, 63)], ids_r)
    all_ids.wait()
    ids = idr[...]
    lane3 = iota((PATCH, BLK, 128), 2)
    holder = jnp.sum(jnp.where(lane3 == HALO, ids, 0), axis=2, keepdims=True)
    seen = jnp.sum(jnp.where((holder == me) & (lane3 < HALO), ids, 0), axis=1)
    seen_f = seen.astype(F32)
    rank = jnp.where(seen > 0, dot(seen_f.astype(BF), low_tri), -1.0)
    listed = jnp.concatenate([hal[0], jnp.zeros((PATCH, 128 - HALO), I32)], axis=1).astype(F32) + 1.0
    wide = iota((PATCH, PATCH * RT), 1)
    mine = wide // RT == iota((PATCH, PATCH * RT), 0)
    spread = jnp.zeros((PATCH, PATCH * RT), F32)
    for r in range(RT):
        node_r = jnp.sum(jnp.where(rank == float(r), listed, 0.0), axis=1, keepdims=True)
        spread = jnp.where(mine & (lax.rem(wide, RT) == r), node_r, spread)
    node_of = jnp.sum(spread, axis=0, keepdims=True).astype(I32) - 1
    amat[...] = hot(iota((NODE, PATCH * RT), 0) == node_of)

    landed(edges_in)
    landed(vecs)
    landed(ed)
    for jr in range(4):
        acc[:, jr * FEAT : (jr + 1) * FEAT] = dot(xe[...], wa[jr, 0]) + vec[pair_of(jr), 0:1, :]
    gain = [jnp.concatenate([vec[k, i : i + 1, :] for k in range(4)], axis=1) for i in (1, 2, 4, 5)]
    landed(rows_in)

    ny = start(weights_y(1))

    def norm(mixed, gain_row, shift_row):
        mean = jnp.sum(mixed, axis=1, keepdims=True) * (1.0 / WIDE)
        spread = jnp.sum(mixed * mixed, axis=1, keepdims=True) * (1.0 / WIDE) - mean * mean
        return (mixed - mean) * lax.rsqrt(spread + EPS) * gain_row + shift_row

    for bb in range(2):
        rows = slice(bb * TILE, (bb + 1) * TILE)
        receiver = rcol[2 * j + bb]
        take = hot(receiver == iota((TILE, HALO), 1))
        mixed = None
        for jr in range(4):
            cols = slice(jr * FEAT, (jr + 1) * FEAT)
            section = dot(xs[ROWS + bb * HALO : ROWS + (bb + 1) * HALO, :], wa[jr, 2]).astype(BF)
            pre = acc[rows, cols] + dot(xs[rows, :], wa[jr, 1]) + dot(take, section)
            hidden = silu(pre).astype(BF)
            term = dot(hidden, wb[jr, 0]).astype(BF).astype(F32)
            mixed = term if mixed is None else mixed + term
        old = xe[rows, :].astype(F32)
        fresh = jnp.where(receiver >= 0, old + norm(mixed, gain[0], gain[1]), old).astype(BF)
        outb[rows, :] = fresh
        rank_row = rank8[pl.ds(2 * j + bb, 1), :][:, 0:HALO]
        which = hot(rank_row == iota((RT, HALO), 0).astype(F32))
        member = hot(rcv[pl.ds(2 * j + bb, 1), :] == iota((HALO, TILE), 0))
        member = dot(which, member).astype(BF)
        tsb[bb * RT : (bb + 1) * RT, :] = dot(member, fresh).astype(BF)

    my_sums = pl.ds(aligned(j * 2 * RT, 2 * RT), 2 * RT)

    def cols_of(dy):
        return pl.ds(aligned(pair_of(dy) * FEAT, FEAT), FEAT)

    sums = start([
        rem(
            tsb.at[:, cols_of(dy)], tsr.at[my_sums], tss.at[dy - 1], tsrr.at[dy - 1],
            (me, pair_of(dy)),
        )
        for dy in (2, 1, 3)
    ])
    tsr[my_sums, :] = tsb[:, my_cols]
    edges_out = start([
        rem(
            outb.at[:, cols_of(dy)], o_e.at[my_edges], oes.at[dy - 1], oer.at[dy - 1],
            (me, pair_of(dy)),
        )
        for dy in (2, 1, 3)
    ])
    keep_e = pltpu.make_async_copy(outb.at[:, my_cols], o_e.at[my_edges], loc.at[10])
    keep_e.start()

    wide_k = iota((1, BLK * RT), 1)
    owner_row = jnp.zeros((1, BLK * RT), I32)
    for b in range(BLK):
        owner_row = jnp.where(wide_k // RT == b, own[b], owner_row)
    rid = iota((PATCH * RT, BLK * RT), 0)
    put = hot((rid // RT == owner_row) & (lax.rem(rid, RT) == lax.rem(wide_k, RT)))
    landed(sums)
    sv[...] = dot(put, tsr[...]).astype(BF)
    my_slot = pl.ds(aligned(me * RT, RT), RT)

    def sum_step(r, carry):
        to = dest(r // 8, lax.rem(r, 8))
        rem(sv.at[pl.ds(aligned(to * RT, RT), RT)], vv.at[my_slot], v2s, v2r, (to, j)).start()
        return carry

    lax.fori_loop(1, PATCH, sum_step, 0)
    vv[my_slot, :] = sv[my_slot, :]

    landed(ny)
    nx = start(weights_x(1))
    landed(nodes_in)
    landed(nx)
    nd = start(weights_d(1))
    landed(nd)
    for jr in range(4):
        acc2[:, jr * FEAT : (jr + 1) * FEAT] = dot(xn[...], wa[jr, 3]) + vec[pair_of(jr), 3:4, :]

    got = vv.at[pl.ds(0, 63 * RT)]
    pltpu.make_async_copy(got, got, v2r).wait()
    mark = len(sent)
    for dy in (2, 1, 3, 0):
        pick_rows = pl.ds(aligned(pair_of(dy) * NROW, NROW), NROW)
        part = dot(amat[pick_rows, :], vv[...]).astype(BF)
        if dy == 0:
            xa[:, my_cols] = part
        else:
            abuf[dy - 1] = part
            start([rem(
                abuf.at[dy - 1], xa.at[:, my_cols], as_.at[dy - 1], ar_.at[dy - 1],
                (me, pair_of(dy)),
            )])
    landed(sent[mark:])
    mixed = None
    for jr in range(4):
        cols = slice(jr * FEAT, (jr + 1) * FEAT)
        hidden = silu(acc2[:, cols] + dot(xa[...], wa[jr, 4])).astype(BF)
        term = dot(hidden, wb[jr, 1]).astype(BF).astype(F32)
        mixed = term if mixed is None else mixed + term
    old = xn[...].astype(F32)
    live = iota((NROW, 1), 0) + j * NROW < cnt[0]
    outn[...] = jnp.where(live, old + norm(mixed, gain[2], gain[3]), old).astype(BF)
    nodes_out = start([
        rem(
            outn.at[:, cols_of(dy)], o_n.at[my_nodes], ons.at[dy - 1], onr.at[dy - 1],
            (me, pair_of(dy)),
        )
        for dy in (2, 1, 3)
    ])
    keep_n = pltpu.make_async_copy(outn.at[:, my_cols], o_n.at[my_nodes], loc.at[11])
    keep_n.start()

    done = picked.at[pl.ds(0, 63 * HALO)]
    pltpu.make_async_copy(done, done, hs).wait()
    pltpu.make_async_copy(idr.at[pl.ds(0, 63)], idr.at[pl.ds(0, 63)], ids_s).wait()
    pltpu.make_async_copy(got, got, v2s).wait()
    for copy in sent:
        copy.wait_send()
    keep_e.wait()
    keep_n.wait()
    landed(edges_out)
    landed(nodes_out)


def shards(
    node_latents, edge_latents, edge_sender, edge_receiver, block_owner, node_counts, halo_nodes,
    w_endpoints, w_edge_in, edge_bias, w_edge_out, edge_gain, edge_shift, w_node_in, node_bias,
    w_node_out, node_gain, node_shift,
):
    row = lambda v: v.reshape(1, FEAT)
    dma = pltpu.SemaphoreType.DMA
    vm = pltpu.VMEM
    scratch = [
        vm((NODE, FEAT), BF), vm((EDGE, 1), I32), vm((EDGE, FEAT), BF), vm((EDGE, FEAT), BF),
        vm((4, SEL, 1), I32), vm((BLK, TILE, 1), I32), vm((BLK, 128), I32), vm((BLK, 128), F32),
        vm((PATCH, BLK, 128), I32), vm((4, 8, FEAT), F32), vm((4, SEL, FEAT), F32),
        vm((3, SEL, FEAT), BF), vm((SEL, WIDE), BF), vm((ROWS, WIDE), BF), vm((NROW, WIDE), BF),
        vm((4, 5, WIDE, FEAT), BF), vm((4, 2, FEAT, WIDE), BF), vm((ROWS, WIDE), F32),
        vm((8, 128), BF), vm((ROWS, WIDE), BF), vm((2 * RT, WIDE), BF), vm((BLK * RT, FEAT), BF),
        vm((PATCH * RT, FEAT), BF), vm((PATCH * RT, FEAT), BF), vm((NODE, PATCH * RT), BF),
        vm((3, NROW, FEAT), BF), vm((NROW, WIDE), BF), vm((NROW, WIDE), F32), vm((NROW, WIDE), BF),
        dma((12,)), dma, dma((4,)), dma, dma, dma((3,)), dma((3,)), dma((3,)), dma((3,)),
        dma((3,)), dma((3,)), dma((4, 3)), dma((4, 3)), dma((4, 3)), dma((4, 3)), dma((4,)),
        dma((4,)), dma((3,)), dma((3,)), dma((3,)), dma((3,)), dma, dma, dma((3,)), dma((3,)),
        dma((3,)), dma((3,)), dma((3,)), dma((3,)),
    ]
    return pl.pallas_call(
        kernel,
        out_shape=(
            jax.ShapeDtypeStruct((NODE, FEAT), BF),
            jax.ShapeDtypeStruct((EDGE, FEAT), BF),
        ),
        in_specs=[ANY, ANY, VM, VM, SM, SM, VM, ANY, ANY, VM, ANY, VM, VM, ANY, VM, ANY, VM, VM],
        out_specs=(ANY, ANY),
        scratch_shapes=scratch,
        compiler_params=pltpu.CompilerParams(
            collective_id=0, has_side_effects=True, vmem_limit_bytes=60 * 2**20
        ),
        name="layer",
    )(
        node_latents, edge_latents, edge_sender, edge_receiver, block_owner, node_counts,
        halo_nodes, jnp.moveaxis(w_endpoints, 1, 0), w_edge_in, row(edge_bias), w_edge_out,
        row(edge_gain), row(edge_shift), w_node_in, row(node_bias), w_node_out, row(node_gain),
        row(node_shift),
    )


def solution(mesh):
    return jax.shard_map(
        shards,
        mesh=mesh,
        in_specs=(
            P("patch", "pair"),
            P("patch", "pair"),
            P("patch", None),
            P("patch", None),
            P("patch"),
            P("patch"),
            P("patch", None, None),
            P(None, None, "pair"),
            P(None, "pair"),
            P("pair"),
            P("pair", None),
            P("pair"),
            P("pair"),
            P(None, None, "pair"),
            P("pair"),
            P("pair", None),
            P("pair"),
            P("pair"),
        ),
        out_specs=(P("patch", "pair"), P("patch", "pair")),
        check_vma=False,
    )
```

```python
import jax
import jax.numpy as jnp
from jax import lax
from jax.experimental import pallas as pl
from jax.experimental.pallas import tpu as pltpu
from jax.sharding import PartitionSpec as P

EPS = 1e-05
MESH = pl.DeviceIdType.MESH
BF = jnp.bfloat16
F32 = jnp.float32
I32 = jnp.int32

NODE = 1024
EDGE = 2048
FEAT = 256
WIDE = 1024
PATCH = 64
HALO = 32
RT = 16
BLK = 8
TILE = 256
ROWS = 2 * TILE
SEL = ROWS + 2 * HALO
NROW = NODE // 4
PICK = 2
ANY = pl.BlockSpec(memory_space=pl.ANY)
VM = pl.BlockSpec(memory_space=pltpu.VMEM)
SM = pl.BlockSpec(memory_space=pltpu.SMEM)


def iota(shape, dim):
    return lax.broadcasted_iota(I32, shape, dim)


def hot(mask):
    return jnp.where(mask, 1.0, 0.0).astype(BF)


def dot(a, b):
    return jnp.dot(a, b, preferred_element_type=F32)


def silu(v):
    return v / (1.0 + jnp.exp(-v))


def aligned(v, n):
    return pl.multiple_of(v, n)


def kernel(
    nl, el, snd, rcv, own, cnt, hal, wep, win, eb, wout, eg, es, wnin, nb, wnout, ng, ns,
    o_n, o_e,
    nl_v, pcol, picked, halo_r, idcol, rcol, idt, rank8, idr, vec, gacc, sbuf, xs,
    xe, xn, wa, wb, wraw, acc, outb, tsb, tsr, sv, vv, amat, putm, abuf, xa, acc2, outn,
    loc, hs, hr, ids_s, ids_r, es_, er_, xns, xnr, vs, vr,
    wys, wyr, wxs, wxr, wzs, wzr, wds, wdr, ss, sr, tss, tsrr, v2s, v2r, as_, ar_, oes, oer,
    ons, onr,
):
    me = lax.axis_index("patch")
    j = lax.axis_index("pair")
    z, x, c = lax.div(me, 8), lax.rem(lax.div(me, 2), 4), lax.rem(me, 2)
    cell = [
        lax.rem(x + t // 2, 4) * 2 + lax.rem(c + t % 2, 2) for t in range(8)
    ]

    def dz_of(m):
        odd = lax.rem(m, 2)
        return lax.rem(odd * lax.div(m + 1, 2) + (1 - odd) * (8 - lax.div(m, 2)), 8)

    def plane_of(m):
        return lax.rem(z + dz_of(m), 8) * 8

    def rem(src, dst, s, r, dev):
        return pltpu.make_async_remote_copy(
            src_ref=src, dst_ref=dst, send_sem=s, recv_sem=r, device_id=dev, device_id_type=MESH
        )

    def each_patch(act):
        def plane(m, first):
            base = plane_of(m)
            for t in range(first, 8):
                act(m, t, base + cell[t])

        def step(m, carry):
            plane(m, 0)
            return carry

        plane(0, 1)
        lax.fori_loop(1, 8, step, 0)

    pairs = [lax.rem(j + dy, 4) for dy in range(4)]

    scope = []

    def phase(name):
        if scope:
            scope.pop().__exit__(None, None, None)
        if name:
            scope.append(jax.named_scope(name))
            scope[-1].__enter__()

    phase("start")
    loads = []

    def load(src, dst):
        copy = pltpu.make_async_copy(src, dst, loc.at[len(loads)])
        copy.start()
        loads.append(copy)
        return copy

    my_cols = pl.ds(aligned(j * FEAT, FEAT), FEAT)
    my_edges = pl.ds(aligned(j * ROWS, ROWS), ROWS)
    my_nodes = pl.ds(aligned(j * NROW, NROW), NROW)
    ld_nl = load(nl, nl_v)

    barrier = pltpu.get_barrier_semaphore()

    def greet(m, t, to):
        pl.semaphore_signal(barrier, inc=1, device_id=(to, j), device_id_type=MESH)

    for dy in (2, 1, 3):
        pl.semaphore_signal(barrier, inc=1, device_id=(me, pairs[dy]), device_id_type=MESH)
    each_patch(greet)
    ld_e = [load(win, wa.at[0, 0]), load(wep, wraw), load(wout, wb.at[0, 0])]
    ld_x = [load(el.at[my_edges], xe.at[:, my_cols]), load(nl.at[my_nodes], xn.at[:, my_cols])]
    ld_n = [load(wnin.at[0], wa.at[0, 3]), load(wnin.at[1], wa.at[0, 4]), load(wnout, wb.at[0, 1])]

    phase("cols")
    for d in range(PATCH):
        pcol[d * HALO : (d + 1) * HALO, :] = hal[0:HALO, d : d + 1]
    ld_nl.wait()
    phase("pick")

    for m in range(0, 8, PICK):
        wanted = [pcol[pl.ds(aligned(plane_of(m + i) * HALO, 256), 256), :] for i in range(PICK)]
        ones = hot(jnp.concatenate(wanted, axis=0) == iota((PICK * 256, NODE), 1))
        picked[m * 256 : (m + PICK) * 256, :] = dot(ones, nl_v[...]).astype(BF)

    phase("wep")
    piece = c * 4 + x
    for copy in ld_e:
        copy.wait()
    my_rows = pl.ds(aligned(piece * 128, 128), 128)
    wa[0, 1, my_rows, :] = wraw[my_rows, 0, :]
    wa[0, 2, my_rows, :] = wraw[my_rows, 1, :]

    phase("barrier")
    pl.semaphore_wait(barrier, PATCH - 1 + 3)
    phase("sends")

    sent = []

    def start(copies):
        for copy in copies:
            copy.start()
        sent.extend(copies)
        return copies

    def landed(copies):
        for copy in copies:
            copy.wait_recv()

    def seg(u, js, base, low, size):
        if u < 5:
            return wa.at[js, u, pl.ds(aligned(base * 128 + low * 64, 64), size * 64)]
        return wb.at[js, u - 5, pl.ds(aligned(base * 32 + low * 16, 16), size * 16)]

    others = pl.ds(1, 3)

    def weights_y(u):
        return start([
            rem(
                seg(u, 0, piece, 0, 2), seg(u, 4 - dy, piece, 0, 2),
                wys.at[u, dy - 1], wyr.at[u, dy - 1], (me, pairs[dy]),
            )
            for dy in (2, 1, 3)
        ])

    right = z * 8 + lax.rem(x + 1, 4) * 2 + c
    left = z * 8 + lax.rem(x + 3, 4) * 2 + c

    def weights_x(u):
        part = seg(u, others, piece, 0, 2)
        return start([
            rem(part, part, wxs.at[u, i], wxr.at[u, i], (to, j)) for i, to in ((0, right), (1, left))
        ])

    def weights_z(u):
        from_left = seg(u, others, c * 4 + lax.rem(x + 3, 4), 0, 1)
        from_right = seg(u, others, c * 4 + lax.rem(x + 1, 4), 1, 1)
        return start([
            rem(from_left, from_left, wzs.at[u, 0], wzr.at[u, 0], (right, j)),
            rem(from_right, from_right, wzs.at[u, 1], wzr.at[u, 1], (left, j)),
        ])

    def weights_d(u):
        part = seg(u, others, c * 4, 0, 8)
        return start([rem(part, part, wds.at[u], wdr.at[u], (z * 8 + x * 2 + 1 - c, j))])

    def send_halo(m, t, to):
        rem(
            picked.at[pl.ds(aligned(m * 256 + cell[t] * HALO, HALO), HALO)],
            halo_r.at[pl.ds(aligned((m * 8 + t) * HALO, HALO), HALO)],
            hs, hr.at[lax.div(m, 2)], (to, j),
        ).start()

    order_e = (0, 1, 2, 5)
    wy = {u: weights_y(u) for u in order_e}
    each_patch(send_halo)
    halo_r[0:HALO, :] = picked[pl.ds(aligned(cell[0] * HALO, HALO), HALO), :]
    part_a, part_b = slice(0, TILE + 2 * HALO), slice(TILE + 2 * HALO, SEL)

    def gather(g):
        slot = g * 16 + iota((1, 512), 1) // HALO
        m = slot // 8
        odd = lax.rem(m, 2)
        dz = odd * ((m + 1) // 2) + (1 - odd) * (8 - m // 2)
        t = lax.rem(slot, 8)
        source = (
            lax.rem(z - dz + 16, 8) * 8 + lax.rem(x - t // 2 + 4, 4) * 2
            + lax.rem(c + lax.rem(t, 2), 2)
        )
        ident = source * HALO + lax.rem(iota((1, 512), 1), HALO)
        low = HALO if g == 0 else 0
        arrived = halo_r.at[pl.ds(g * 512 + low, 512 - low)]
        pltpu.make_async_copy(arrived, arrived, hr.at[g]).wait()
        table = halo_r.at[g * 512 : (g + 1) * 512]
        if g < 3:
            for dy in (2, 1, 3, 0):
                part = dot(hot(idcol[pairs[dy]] == ident), table[...])
                gacc[dy] = part if g == 0 else gacc[dy] + part
            return []
        copies = []
        for half, rows in enumerate((part_a, part_b)):
            for dy in (2, 1, 3, 0):
                part = dot(hot(idcol[pairs[dy], rows, :] == ident), table[...])
                part = (gacc[dy, rows, :] + part).astype(BF)
                if dy == 0:
                    xs[rows, my_cols] = part
                else:
                    sbuf[dy - 1, rows, :] = part
                    copies.append(rem(
                        sbuf.at[dy - 1, rows], xs.at[rows, my_cols], ss.at[half, dy - 1],
                        sr.at[half, dy - 1], (me, pairs[dy]),
                    ))
                    start(copies[-1:])
        return copies

    wx, wz, wd = {}, {}, {}

    def wy_to_x(u):
        landed(wy[u])
        wx[u] = weights_x(u)

    def x_to_z(u):
        landed(wx[u])
        wz[u] = weights_z(u)

    def z_to_d(u):
        landed(wz[u])
        wd[u] = weights_d(u)

    def block_ids():
        snd_t = snd[...].T
        rcv_t = rcv[...].T
        lane = iota((TILE, 128), 1)
        for b in range(BLK):
            g, low = b // 2, (b % 2) * (TILE + 2 * HALO)
            idcol[g, low : low + TILE, :] = snd_t[:, b : b + 1]
            low = TILE + (b % 2) * HALO
            idcol[g, low : low + HALO, :] = iota((HALO, 1), 0) + own[b] * HALO
            rcol[b] = rcv_t[:, b : b + 1]
            seen = jnp.max(jnp.where(rcv_t[:, b : b + 1] == lane, 1, 0), axis=0, keepdims=True)
            idt[b : b + 1, :] = jnp.where(iota((1, 128), 1) == HALO, own[b], seen)

    phase("idcols")
    block_ids()
    for i, ref in enumerate((eb, eg, es, nb, ng, ns)):
        vec[j, i : i + 1, :] = ref[...]
    phase("vecs")
    vecs = start([
        rem(vec.at[j], vec.at[j], vs.at[dy - 1], vr.at[dy - 1], (me, pairs[dy]))
        for dy in (2, 1, 3)
    ])

    phase("wy0")
    wy_to_x(0)
    phase("wep2")

    def split(k, carry):
        rows = pl.ds(aligned(lax.rem(piece + k, 8) * 128, 128), 128)
        wa[0, 1, rows, :] = wraw[rows, 0, :]
        wa[0, 2, rows, :] = wraw[rows, 1, :]
        return carry

    lax.fori_loop(1, 8, split, 0)
    phase("g0")
    gather(0)
    phase("wy1")
    wy_to_x(1)
    phase("wy2")
    wy_to_x(2)
    phase("g1")
    gather(1)
    phase("wy5")
    wy_to_x(5)
    phase("edgesin")
    edges_in = start([
        rem(
            el.at[pl.ds(aligned(pairs[dy] * ROWS, ROWS), ROWS)], xe.at[:, my_cols],
            es_.at[dy - 1], er_.at[dy - 1], (me, pairs[dy]),
        )
        for dy in (2, 1, 3)
    ])
    phase("x0")
    x_to_z(0)
    phase("g2")
    gather(2)
    phase("ny")
    for copy in ld_n:
        copy.wait()
    for u in (3, 4):
        wy[u] = weights_y(u)
    phase("x1")
    x_to_z(1)
    phase("g3")
    rows_in = gather(3)
    phase("ldn")
    for copy in ld_x:
        copy.wait()
    def send_ids(m, t, to):
        rem(idt, idr.at[me], ids_s, ids_r, (to, j)).start()

    each_patch(send_ids)
    idr[me] = idt[...]

    phase("z0")
    z_to_d(0)
    phase("x2")
    x_to_z(2)
    phase("z1")
    z_to_d(1)

    phase("tables")
    low_tri = hot(iota((128, 128), 0) < iota((128, 128), 1))
    live8 = jnp.where(iota((BLK, 128), 1) < HALO, idt[...], 0)
    rank8[...] = jnp.where(live8 > 0, dot(live8.astype(F32).astype(BF), low_tri), -1.0)
    all_ids = pltpu.make_async_copy(idr.at[pl.ds(0, 63)], idr.at[pl.ds(0, 63)], ids_r)
    all_ids.wait()
    ids = idr[...]
    lane3 = iota((PATCH, BLK, 128), 2)
    holder = jnp.sum(jnp.where(lane3 == HALO, ids, 0), axis=2, keepdims=True)
    seen = jnp.sum(jnp.where((holder == me) & (lane3 < HALO), ids, 0), axis=1)
    rank = jnp.where(seen > 0, dot(seen.astype(F32).astype(BF), low_tri), -1.0)
    listed = jnp.concatenate([hal[...], jnp.zeros((HALO, PATCH), I32)], axis=1)
    listed = jnp.concatenate([listed, jnp.zeros((128 - HALO, 128), I32)], axis=0)
    listed = listed.T[0:PATCH].astype(F32) + 1.0
    wide = iota((PATCH, PATCH * RT), 1)
    mine = wide // RT == iota((PATCH, PATCH * RT), 0)
    spread = jnp.zeros((PATCH, PATCH * RT), F32)
    for r in range(RT):
        node_r = jnp.sum(jnp.where(rank == float(r), listed, 0.0), axis=1, keepdims=True)
        spread = jnp.where(mine & (lax.rem(wide, RT) == r), node_r, spread)
    node_of = jnp.sum(spread, axis=0, keepdims=True).astype(I32) - 1
    amat[...] = hot(iota((NODE, PATCH * RT), 0) == node_of)
    wide_k = iota((1, BLK * RT), 1)
    owner_row = jnp.zeros((1, BLK * RT), I32)
    for b in range(BLK):
        owner_row = jnp.where(wide_k // RT == b, own[b], owner_row)
    rid = iota((PATCH * RT, BLK * RT), 0)
    putm[...] = hot((rid // RT == owner_row) & (lax.rem(rid, RT) == lax.rem(wide_k, RT)))

    phase("x5")
    x_to_z(5)
    phase("z2")
    z_to_d(2)
    phase("w_edges")
    landed(edges_in)
    landed(vecs)
    phase("w_d0")
    landed(wd[0])
    phase("edge1")
    for jr in range(4):
        acc[:, jr * FEAT : (jr + 1) * FEAT] = dot(xe[...], wa[jr, 0]) + vec[pairs[jr], 0:1, :]
    gain = [jnp.concatenate([vec[k, i : i + 1, :] for k in range(4)], axis=1) for i in (1, 2, 4, 5)]
    phase("z5")
    z_to_d(5)
    phase("n34")
    wy_to_x(3)
    wy_to_x(4)
    phase("w_rows0")
    landed(rows_in[0:3])
    wy[6] = weights_y(6)
    phase("w_d")
    landed(wd[1])
    landed(wd[2])
    landed(wd[5])

    def norm(mixed, gain_row, shift_row):
        mean = jnp.sum(mixed, axis=1, keepdims=True) * (1.0 / WIDE)
        spread = jnp.sum(mixed * mixed, axis=1, keepdims=True) * (1.0 / WIDE) - mean * mean
        return (mixed - mean) * lax.rsqrt(spread + EPS) * gain_row + shift_row

    section = [dot(xs[TILE : TILE + 2 * HALO, :], wa[k, 2]).astype(BF) for k in range(4)]
    for bb in range(2):
        if bb:
            phase("w_rows1")
            landed(rows_in[3:6])
        phase("edge2_%d" % bb)
        rows = slice(bb * TILE, (bb + 1) * TILE)
        in_xs = slice(bb * (TILE + 2 * HALO), bb * (TILE + 2 * HALO) + TILE)
        receiver = rcol[2 * j + bb]
        take = hot(receiver == iota((TILE, HALO), 1))
        mixed = None
        for jr in range(4):
            cols = slice(jr * FEAT, (jr + 1) * FEAT)
            pre = acc[rows, cols] + dot(xs[in_xs, :], wa[jr, 1])
            pre = pre + dot(take, section[jr][bb * HALO : (bb + 1) * HALO, :])
            hidden = silu(pre).astype(BF)
            term = dot(hidden, wb[jr, 0]).astype(BF).astype(F32)
            mixed = term if mixed is None else mixed + term
        old = xe[rows, :].astype(F32)
        fresh = jnp.where(receiver >= 0, old + norm(mixed, gain[0], gain[1]), old).astype(BF)
        outb[rows, :] = fresh
        rank_row = rank8[pl.ds(2 * j + bb, 1), :][:, 0:HALO]
        which = hot(rank_row == iota((RT, HALO), 0).astype(F32))
        member = hot(rcv[pl.ds(2 * j + bb, 1), :] == iota((HALO, TILE), 0))
        member = dot(which, member).astype(BF)
        tsb[bb * RT : (bb + 1) * RT, :] = dot(member, fresh).astype(BF)

    phase("esend")
    my_sums = pl.ds(aligned(j * 2 * RT, 2 * RT), 2 * RT)

    def cols_of(dy):
        return pl.ds(aligned(pairs[dy] * FEAT, FEAT), FEAT)

    sums = start([
        rem(
            tsb.at[:, cols_of(dy)], tsr.at[my_sums], tss.at[dy - 1], tsrr.at[dy - 1],
            (me, pairs[dy]),
        )
        for dy in (2, 1, 3)
    ])
    tsr[my_sums, :] = tsb[:, my_cols]
    phase("w_sums")
    landed(sums)
    phase("sumsend")
    sv[...] = dot(putm[...], tsr[...]).astype(BF)
    my_slot = pl.ds(aligned(me * RT, RT), RT)

    def send_sum(m, t, to):
        rem(sv.at[pl.ds(aligned(to * RT, RT), RT)], vv.at[my_slot], v2s, v2r, (to, j)).start()

    each_patch(send_sum)
    vv[my_slot, :] = sv[my_slot, :]

    phase("eout")
    nodes_in = start([
        rem(
            nl.at[pl.ds(aligned(pairs[dy] * NROW, NROW), NROW)], xn.at[:, my_cols],
            xns.at[dy - 1], xnr.at[dy - 1], (me, pairs[dy]),
        )
        for dy in (2, 1, 3)
    ])
    edges_out = start([
        rem(
            outb.at[:, cols_of(dy)], o_e.at[my_edges], oes.at[dy - 1], oer.at[dy - 1],
            (me, pairs[dy]),
        )
        for dy in (2, 1, 3)
    ])
    keep_e = pltpu.make_async_copy(outb.at[:, my_cols], o_e.at[my_edges], loc.at[10])
    keep_e.start()

    phase("w_ny")
    wy_to_x(6)
    phase("w_nx")
    for u in (3, 4, 6):
        x_to_z(u)
    phase("w_nz")
    for u in (3, 4, 6):
        z_to_d(u)
    phase("w_nin")
    landed(nodes_in)
    phase("w_nd")
    for u in (3, 4, 6):
        landed(wd[u])
    phase("node1")
    for jr in range(4):
        acc2[:, jr * FEAT : (jr + 1) * FEAT] = dot(xn[...], wa[jr, 3]) + vec[pairs[jr], 3:4, :]

    phase("w_vv")
    got = vv.at[pl.ds(0, 63 * RT)]
    pltpu.make_async_copy(got, got, v2r).wait()
    phase("agg")
    half_n = NROW // 2
    agg_in = []
    for h in range(2):
        rows = slice(h * half_n, (h + 1) * half_n)
        for dy in (2, 1, 3, 0):
            from_rows = pl.ds(aligned(pairs[dy] * NROW + h * half_n, half_n), half_n)
            part = dot(amat[from_rows, :], vv[...]).astype(BF)
            if dy == 0:
                xa[rows, my_cols] = part
            else:
                abuf[dy - 1, rows, :] = part
                agg_in.append(rem(
                    abuf.at[dy - 1, rows], xa.at[rows, my_cols], as_.at[h, dy - 1],
                    ar_.at[h, dy - 1], (me, pairs[dy]),
                ))
                start(agg_in[-1:])
    nodes_out = []
    keep_n = []
    for h in range(2):
        phase("w_agg%d" % h)
        landed(agg_in[3 * h : 3 * h + 3])
        phase("node2_%d" % h)
        rows = slice(h * half_n, (h + 1) * half_n)
        mixed = None
        for jr in range(4):
            cols = slice(jr * FEAT, (jr + 1) * FEAT)
            hidden = silu(acc2[rows, cols] + dot(xa[rows, :], wa[jr, 4])).astype(BF)
            term = dot(hidden, wb[jr, 1]).astype(BF).astype(F32)
            mixed = term if mixed is None else mixed + term
        old = xn[rows, :].astype(F32)
        live = iota((half_n, 1), 0) + (j * NROW + h * half_n) < cnt[0]
        outn[rows, :] = jnp.where(live, old + norm(mixed, gain[2], gain[3]), old).astype(BF)
        to_rows = pl.ds(aligned(j * NROW + h * half_n, half_n), half_n)
        nodes_out.extend(start([
            rem(
                outn.at[rows, cols_of(dy)], o_n.at[to_rows], ons.at[h, dy - 1], onr.at[h, dy - 1],
                (me, pairs[dy]),
            )
            for dy in (2, 1, 3)
        ]))
        copy = pltpu.make_async_copy(outn.at[rows, my_cols], o_n.at[to_rows], loc.at[11 + h])
        copy.start()
        keep_n.append(copy)

    phase("end_s")
    done = picked.at[pl.ds(0, 63 * HALO)]
    pltpu.make_async_copy(done, done, hs).wait()
    pltpu.make_async_copy(idr.at[pl.ds(0, 63)], idr.at[pl.ds(0, 63)], ids_s).wait()
    pltpu.make_async_copy(got, got, v2s).wait()
    for copy in sent:
        copy.wait_send()
    keep_e.wait()
    for copy in keep_n:
        copy.wait()
    phase("end_e")
    landed(edges_out)
    phase("end_n")
    landed(nodes_out)
    phase(None)


def shards(
    node_latents, edge_latents, edge_sender, edge_receiver, block_owner, node_counts, halo_nodes,
    w_endpoints, w_edge_in, edge_bias, w_edge_out, edge_gain, edge_shift, w_node_in, node_bias,
    w_node_out, node_gain, node_shift,
):
    row = lambda v: v.reshape(1, FEAT)
    dma = pltpu.SemaphoreType.DMA
    vm = pltpu.VMEM
    scratch = [
        vm((NODE, FEAT), BF), vm((EDGE, 1), I32), vm((EDGE, FEAT), BF), vm((EDGE, FEAT), BF),
        vm((4, SEL, 1), I32), vm((BLK, TILE, 1), I32), vm((BLK, 128), I32), vm((BLK, 128), F32),
        vm((PATCH, BLK, 128), I32), vm((4, 8, FEAT), F32), vm((4, SEL, FEAT), F32),
        vm((3, SEL, FEAT), BF), vm((SEL, WIDE), BF), vm((ROWS, WIDE), BF), vm((NROW, WIDE), BF),
        vm((4, 5, WIDE, FEAT), BF), vm((4, 2, FEAT, WIDE), BF), vm((WIDE, 2, FEAT), BF),
        vm((ROWS, WIDE), F32), vm((ROWS, WIDE), BF), vm((2 * RT, WIDE), BF),
        vm((BLK * RT, FEAT), BF), vm((PATCH * RT, FEAT), BF), vm((PATCH * RT, FEAT), BF),
        vm((NODE, PATCH * RT), BF), vm((PATCH * RT, BLK * RT), BF), vm((3, NROW, FEAT), BF),
        vm((NROW, WIDE), BF), vm((NROW, WIDE), F32), vm((NROW, WIDE), BF),
        dma((13,)), dma, dma((4,)), dma, dma, dma((3,)), dma((3,)), dma((3,)), dma((3,)),
        dma((3,)), dma((3,)), dma((7, 3)), dma((7, 3)), dma((7, 2)), dma((7, 2)), dma((7, 2)),
        dma((7, 2)), dma((7,)), dma((7,)), dma((2, 3)), dma((2, 3)), dma((3,)), dma((3,)), dma,
        dma, dma((2, 3)), dma((2, 3)), dma((3,)), dma((3,)), dma((2, 3)), dma((2, 3)),
    ]
    return pl.pallas_call(
        kernel,
        out_shape=(
            jax.ShapeDtypeStruct((NODE, FEAT), BF),
            jax.ShapeDtypeStruct((EDGE, FEAT), BF),
        ),
        in_specs=[ANY, ANY, VM, VM, SM, SM, VM, ANY, ANY, VM, ANY, VM, VM, ANY, VM, ANY, VM, VM],
        out_specs=(ANY, ANY),
        scratch_shapes=scratch,
        compiler_params=pltpu.CompilerParams(
            collective_id=0, has_side_effects=True, vmem_limit_bytes=60 * 2**20
        ),
        name="layer",
    )(
        node_latents, edge_latents, edge_sender, edge_receiver, block_owner, node_counts,
        halo_nodes[0].T, w_endpoints, w_edge_in, row(edge_bias), w_edge_out,
        row(edge_gain), row(edge_shift), w_node_in, row(node_bias), w_node_out, row(node_gain),
        row(node_shift),
    )


def solution(mesh):
    return jax.shard_map(
        shards,
        mesh=mesh,
        in_specs=(
            P("patch", "pair"),
            P("patch", "pair"),
            P("patch", None),
            P("patch", None),
            P("patch"),
            P("patch"),
            P("patch", None, None),
            P(None, None, "pair"),
            P(None, "pair"),
            P("pair"),
            P("pair", None),
            P("pair"),
            P("pair"),
            P(None, None, "pair"),
            P("pair"),
            P("pair", None),
            P("pair"),
            P("pair"),
        ),
        out_specs=(P("patch", "pair"), P("patch", "pair")),
        check_vma=False,
    )
```

```python
import jax
import jax.numpy as jnp
from jax import lax
from jax.experimental import pallas as pl
from jax.experimental.pallas import tpu as pltpu
from jax.sharding import PartitionSpec as P

EPS = 1e-05
MESH = pl.DeviceIdType.MESH
BF = jnp.bfloat16
F32 = jnp.float32
I32 = jnp.int32

NODE = 1024
EDGE = 2048
FEAT = 256
WIDE = 1024
PATCH = 64
HALO = 32
RT = 16
BLK = 8
TILE = 256
ROWS = 2 * TILE
SEL = ROWS + 2 * HALO
NROW = NODE // 4
PICK = 2
CUT = 512
ANY = pl.BlockSpec(memory_space=pl.ANY)
VM = pl.BlockSpec(memory_space=pltpu.VMEM)


def iota(shape, dim):
    return lax.broadcasted_iota(I32, shape, dim)


def hot(mask):
    return jnp.where(mask, 1.0, 0.0).astype(BF)


def dot(a, b):
    return jnp.dot(a, b, preferred_element_type=F32)


def silu(v):
    return v / (1.0 + jnp.exp(-v))


def aligned(v, n):
    return pl.multiple_of(v, n)


def kernel(
    nl, el, snd_h, rcv_h, own_h, cnt_h, hal_h, wep, win, eb, wout, eg, es, wnin, nb, wnout, ng, ns,
    o_n, o_e,
    own, cnt, snd, rcv, hal, nl_v, pcol, picked, halo_r, idcol, rcol, idt, idm, rank8, idr, vec, gacc, sbuf, xs,
    xe, xn, wa, wb, wraw, acc, hid, outb, tsb, tsr, sv, vv, amat, putm, abuf, xa, acc2, outn,
    loc, hs, hr, ids_s, ids_r, es_, er_, xns, xnr, vs, vr,
    wys, wyr, wxs, wxr, wzs, wzr, wrs, wrr, wds, wdr, ss, sr, tss, tsrr, v2s, v2r, as_, ar_, oes, oer,
    ons, onr,
):
    me = lax.axis_index("patch")
    j = lax.axis_index("pair")
    z, x, c = lax.div(me, 8), lax.rem(lax.div(me, 2), 4), lax.rem(me, 2)
    cell = [
        lax.rem(x + t // 2, 4) * 2 + lax.rem(c + t % 2, 2) for t in range(8)
    ]

    def dz_of(m):
        odd = lax.rem(m, 2)
        return lax.rem(odd * lax.div(m + 1, 2) + (1 - odd) * (8 - lax.div(m, 2)), 8)

    def plane_of(m):
        return lax.rem(z + dz_of(m), 8) * 8

    def rem(src, dst, s, r, dev):
        return pltpu.make_async_remote_copy(
            src_ref=src, dst_ref=dst, send_sem=s, recv_sem=r, device_id=dev, device_id_type=MESH
        )

    def each_patch(act):
        def plane(m, first):
            base = plane_of(m)
            for t in range(first, 8):
                act(m, t, base + cell[t])

        def step(m, carry):
            plane(m, 0)
            return carry

        plane(0, 1)
        lax.fori_loop(1, 8, step, 0)

    pairs = [lax.rem(j + dy, 4) for dy in range(4)]

    scope = []

    def phase(name):
        if scope:
            scope.pop().__exit__(None, None, None)
        if name:
            scope.append(jax.named_scope(name))
            scope[-1].__enter__()

    phase("start")
    loads = []

    def load(src, dst):
        copy = pltpu.make_async_copy(src, dst, loc.at[len(loads)])
        copy.start()
        loads.append(copy)
        return copy

    my_cols = pl.ds(aligned(j * FEAT, FEAT), FEAT)
    my_edges = pl.ds(aligned(j * ROWS, ROWS), ROWS)
    my_nodes = pl.ds(aligned(j * NROW, NROW), NROW)
    ld_hal = load(hal_h, hal)
    ld_nl = load(nl, nl_v)

    barrier = pltpu.get_barrier_semaphore()

    def greet(m, t, to):
        pl.semaphore_signal(barrier, inc=1, device_id=(to, j), device_id_type=MESH)

    def greet_plane(m, carry):
        base = plane_of(7 - m)
        for t in range(8):
            greet(7 - m, t, base + cell[t])
        return carry

    for dy in (2, 1, 3):
        pl.semaphore_signal(barrier, inc=1, device_id=(me, pairs[dy]), device_id_type=MESH)
    lax.fori_loop(0, 7, greet_plane, 0)
    for t in range(1, 8):
        greet(0, t, plane_of(0) + cell[t])
    ld_e = [load(win, wa.at[0, 0]), load(wep, wraw), load(wout, wb.at[0, 0])]
    ld_i = [load(snd_h, snd), load(rcv_h, rcv), load(own_h, own), load(cnt_h, cnt)]
    ld_i += [
        load(ref, vec.at[j, pl.ds(i, 1)]) for i, ref in enumerate((eb, eg, es, nb, ng, ns))
    ]
    ld_x = [load(el.at[my_edges], xe.at[:, my_cols]), load(nl.at[my_nodes], xn.at[:, my_cols])]
    ld_n = [load(wnin.at[0], wa.at[0, 3]), load(wnin.at[1], wa.at[0, 4]), load(wnout, wb.at[0, 1])]

    phase("cols")
    ld_hal.wait()
    for d in range(PATCH):
        pcol[d * HALO : (d + 1) * HALO, :] = hal[0:HALO, d : d + 1]
    ld_nl.wait()
    phase("pick")

    for m in range(0, 8, PICK):
        wanted = [pcol[pl.ds(aligned(plane_of(m + i) * HALO, 256), 256), :] for i in range(PICK)]
        ones = hot(jnp.concatenate(wanted, axis=0) == iota((PICK * 256, NODE), 1))
        picked[m * 256 : (m + PICK) * 256, :] = dot(ones, nl_v[...]).astype(BF)

    phase("wep")
    piece = c * 4 + x
    for copy in ld_e:
        copy.wait()
    my_rows = pl.ds(aligned(piece * 128, 128), 128)
    wa[0, 1, my_rows, :] = wraw[my_rows, 0, :]
    wa[0, 2, my_rows, :] = wraw[my_rows, 1, :]

    phase("barrier")
    pl.semaphore_wait(barrier, PATCH - 1 + 3)
    phase("sends")

    sent = []

    def start(copies):
        for copy in copies:
            copy.start()
        sent.extend(copies)
        return copies

    def landed(copies):
        for copy in copies:
            copy.wait_recv()

    def seg(u, js, base, low, size):
        if u < 5:
            return wa.at[js, u, pl.ds(aligned(base * 128 + low * 64, 64), size * 64)]
        rows = pl.ds(aligned(base * 32 + low * 16, 16), size * 16)
        cols = pl.ds(0, CUT) if u < 7 else pl.ds(CUT, WIDE - CUT)
        return wb.at[js, (u + 1) % 2, rows, cols]

    def thin(u, js):
        rows = pl.ds(aligned((c * 8 + z) * 16, 16), 16)
        return wb.at[js, (u + 1) % 2, rows, pl.ds(0, CUT)]

    others = pl.ds(1, 3)

    def weights_y(u):
        return start([
            rem(
                thin(u, 0) if u in (5, 6) else seg(u, 0, piece, 0, 2),
                thin(u, 4 - dy) if u in (5, 6) else seg(u, 4 - dy, piece, 0, 2),
                wys.at[u, dy - 1], wyr.at[u, dy - 1], (me, pairs[dy]),
            )
            for dy in (2, 1, 3)
        ])

    right = z * 8 + lax.rem(x + 1, 4) * 2 + c
    left = z * 8 + lax.rem(x + 3, 4) * 2 + c

    def weights_x(u):
        part = seg(u, others, piece, 0, 2)
        return start([
            rem(part, part, wxs.at[u, i], wxr.at[u, i], (to, j)) for i, to in ((0, right), (1, left))
        ])

    def weights_z(u):
        from_left = seg(u, others, c * 4 + lax.rem(x + 3, 4), 0, 1)
        from_right = seg(u, others, c * 4 + lax.rem(x + 1, 4), 1, 1)
        return start([
            rem(from_left, from_left, wzs.at[u, 0], wzr.at[u, 0], (right, j)),
            rem(from_right, from_right, wzs.at[u, 1], wzr.at[u, 1], (left, j)),
        ])

    def weights_round(u):
        return start([
            rem(
                thin(u, others), thin(u, others), wrs.at[u - 5, dz - 1], wrr.at[u - 5, dz - 1],
                (lax.rem(z + dz, 8) * 8 + x * 2 + c, j),
            )
            for dz in (4, 3, 5, 2, 6, 1, 7)
        ])

    def weights_d(u):
        part = seg(u, others, c * 4, 0, 8)
        return start([rem(part, part, wds.at[u], wdr.at[u], (z * 8 + x * 2 + 1 - c, j))])

    def send_halo(m, t, to):
        rem(
            picked.at[pl.ds(aligned(m * 256 + cell[t] * HALO, HALO), HALO)],
            halo_r.at[pl.ds(aligned((m * 8 + t) * HALO, HALO), HALO)],
            hs, hr.at[lax.div(m, 2)], (to, j),
        ).start()

    order_e = (0, 1, 2, 7, 5)
    wy = {0: weights_y(0)}
    each_patch(send_halo)
    halo_r[0:HALO, :] = picked[pl.ds(aligned(cell[0] * HALO, HALO), HALO), :]
    wx, wz, wd = {}, {}, {}

    part_a, part_b = slice(0, TILE + 2 * HALO), slice(TILE + 2 * HALO, SEL)

    def gather(g):
        slot = g * 16 + iota((1, 512), 1) // HALO
        m = slot // 8
        odd = lax.rem(m, 2)
        dz = odd * ((m + 1) // 2) + (1 - odd) * (8 - m // 2)
        t = lax.rem(slot, 8)
        source = (
            lax.rem(z - dz + 16, 8) * 8 + lax.rem(x - t // 2 + 4, 4) * 2
            + lax.rem(c + lax.rem(t, 2), 2)
        )
        ident = source * HALO + lax.rem(iota((1, 512), 1), HALO)
        low = HALO if g == 0 else 0
        arrived = halo_r.at[pl.ds(g * 512 + low, 512 - low)]
        pltpu.make_async_copy(arrived, arrived, hr.at[g]).wait()
        if g == 3:
            wz[5] = weights_round(5)
        table = halo_r.at[g * 512 : (g + 1) * 512]
        if g < 3:
            for dy in (2, 1, 3, 0):
                part = dot(hot(idcol[pairs[dy]] == ident), table[...])
                gacc[dy] = part if g == 0 else gacc[dy] + part
            return []
        copies = []
        for half, rows in enumerate((part_a, part_b)):
            for dy in (2, 1, 3, 0):
                part = dot(hot(idcol[pairs[dy], rows, :] == ident), table[...])
                part = (gacc[dy, rows, :] + part).astype(BF)
                if dy == 0:
                    xs[rows, my_cols] = part
                else:
                    sbuf[dy - 1, rows, :] = part
                    copies.append(rem(
                        sbuf.at[dy - 1, rows], xs.at[rows, my_cols], ss.at[half, dy - 1],
                        sr.at[half, dy - 1], (me, pairs[dy]),
                    ))
                    start(copies[-1:])
        return copies

    def wy_to_x(u):
        landed(wy[u])
        wx[u] = weights_x(u)

    def x_to_z(u):
        landed(wx[u])
        wz[u] = weights_z(u)

    def z_to_d(u):
        landed(wz[u])
        wd[u] = weights_d(u)

    def block_ids():
        snd_t = snd[...].T
        rcv_t = rcv[...].T
        lane = iota((TILE, 128), 1)
        for b in range(BLK):
            g, low = b // 2, 2 * HALO + (b % 2) * TILE
            idcol[g, low : low + TILE, :] = snd_t[:, b : b + 1]
            low = (b % 2) * HALO
            idcol[g, low : low + HALO, :] = iota((HALO, 1), 0) + own[b] * HALO
            rcol[b] = rcv_t[:, b : b + 1]
            seen = jnp.max(jnp.where(rcv_t[:, b : b + 1] == lane, 1, 0), axis=0, keepdims=True)
            idt[b : b + 1, :] = seen

    phase("idcols")
    for copy in ld_i:
        copy.wait()
    block_ids()
    phase("vecs")
    for u in order_e[1:]:
        wy[u] = weights_y(u)
    vecs = start([
        rem(vec.at[j], vec.at[j], vs.at[dy - 1], vr.at[dy - 1], (me, pairs[dy]))
        for dy in (2, 1, 3)
    ])

    phase("wy0")
    wy_to_x(0)
    phase("wep2")

    def split(k, carry):
        rows = pl.ds(aligned(lax.rem(piece + k, 8) * 128, 128), 128)
        wa[0, 1, rows, :] = wraw[rows, 0, :]
        wa[0, 2, rows, :] = wraw[rows, 1, :]
        return carry

    lax.fori_loop(1, 8, split, 0)
    phase("edgesin")
    edges_in = start([
        rem(
            el.at[pl.ds(aligned(pairs[dy] * ROWS, ROWS), ROWS)], xe.at[:, my_cols],
            es_.at[dy - 1], er_.at[dy - 1], (me, pairs[dy]),
        )
        for dy in (2, 1, 3)
    ])
    phase("g0")
    gather(0)
    phase("wy1")
    wy_to_x(1)
    phase("wy2")
    wy_to_x(2)
    for copy in ld_n:
        copy.wait()
    for u in (3, 6):
        wy[u] = weights_y(u)
    phase("g1")
    gather(1)
    phase("wy5")
    landed(wy[5])
    wy_to_x(7)
    phase("x0")
    x_to_z(0)
    phase("g2")
    gather(2)
    phase("ny")
    phase("x1")
    x_to_z(1)
    phase("g3")
    rows_in = gather(3)
    phase("ldn")
    for copy in ld_x:
        copy.wait()
    phase("z0")
    z_to_d(0)
    phase("x2")
    x_to_z(2)
    phase("x7")
    x_to_z(7)
    phase("z1")
    z_to_d(1)

    phase("tables")
    low_tri = hot(iota((128, 128), 0) < iota((128, 128), 1))
    live8 = jnp.where(iota((BLK, 128), 1) < HALO, idt[...], 0)
    lane8 = iota((BLK, 128), 1)
    bit = lax.shift_left(jnp.ones((BLK, 128), I32), lax.rem(lane8, 16))
    bits = [
        jnp.sum(jnp.where(lane8 // 16 == k, live8 * bit, 0), axis=1, keepdims=True) for k in range(2)
    ]
    lane1 = iota((1, 128), 1)
    message = jnp.zeros((1, 128), I32)
    for b in range(BLK):
        message = jnp.where(lane1 == b * 16, own[b], message)
        for k in range(2):
            message = jnp.where(lane1 == b * 16 + 1 + k, bits[k][b : b + 1, :], message)
    idm[...] = message
    def send_ids(m, t, to):
        rem(idm, idr.at[me], ids_s, ids_r, (to, j)).start()

    each_patch(send_ids)
    idr[me] = idm[...]

    rank8[...] = jnp.where(live8 > 0, dot(live8.astype(F32).astype(BF), low_tri), -1.0)
    wide_k = iota((1, BLK * RT), 1)
    owner_row = jnp.zeros((1, BLK * RT), I32)
    for b in range(BLK):
        owner_row = jnp.where(wide_k // RT == b, own[b], owner_row)
    rid = iota((PATCH * RT, BLK * RT), 0)
    putm[...] = hot((rid // RT == owner_row) & (lax.rem(rid, RT) == lax.rem(wide_k, RT)))

    phase("z2")
    z_to_d(2)
    phase("z5w")
    landed(wz[5])
    wd[5] = weights_d(5)
    phase("w_edges")
    landed(edges_in)
    landed(vecs)
    phase("w_d0")
    landed(wd[0])
    phase("edge1")
    for jr in range(4):
        acc[:, jr * FEAT : (jr + 1) * FEAT] = dot(xe[...], wa[jr, 0]) + vec[pairs[jr], 0:1, :]
    gain = [jnp.concatenate([vec[k, i : i + 1, :] for k in range(4)], axis=1) for i in (1, 2, 4, 5)]
    phase("z7")
    z_to_d(7)
    phase("n3")
    landed(wy[6])
    wz[6] = weights_round(6)
    wy_to_x(3)
    phase("w_rows0")
    landed(rows_in[0:3])
    phase("w_d")
    landed(wd[1])
    landed(wd[2])
    landed(wd[5])
    landed(wd[7])

    def norm(mixed, gain_row, shift_row):
        mean = jnp.sum(mixed, axis=1, keepdims=True) * (1.0 / WIDE)
        spread = jnp.sum(mixed * mixed, axis=1, keepdims=True) * (1.0 / WIDE) - mean * mean
        return (mixed - mean) * lax.rsqrt(spread + EPS) * gain_row + shift_row

    phase("section")
    section = [dot(xs[0 : 2 * HALO, :], wa[k, 2]).astype(BF) for k in range(4)]
    phase("w_rows1")
    both = jnp.concatenate([rcol[2 * j], rcol[2 * j + 1]], axis=0)
    lane2 = iota((ROWS, 2 * HALO), 1)
    base2 = (iota((ROWS, 2 * HALO), 0) // TILE) * HALO
    take = hot((both >= 0) & (both + base2 == lane2))
    landed(rows_in[3:6])
    for u in (4, 8):
        wy[u] = weights_y(u)
    phase("edge2a")
    for k in range(4):
        cols = slice(k * FEAT, (k + 1) * FEAT)
        pre = acc[:, cols] + dot(xs[2 * HALO :, :], wa[k, 1]) + dot(take, section[k])
        hid[:, cols] = silu(pre).astype(BF)
    phase("x346")
    phase("edge2b")
    first = jnp.zeros((ROWS, 1), F32)
    second = jnp.zeros((ROWS, 1), F32)
    for n in range(4):
        cols = slice(n * FEAT, (n + 1) * FEAT)
        mixed = None
        for k in range(4):
            term = dot(hid[:, k * FEAT : (k + 1) * FEAT], wb[k, 0, :, cols]).astype(BF).astype(F32)
            mixed = term if mixed is None else mixed + term
        acc[:, cols] = mixed
        first = first + jnp.sum(mixed, axis=1, keepdims=True)
        second = second + jnp.sum(mixed * mixed, axis=1, keepdims=True)
    mean = first * (1.0 / WIDE)
    scale = lax.rsqrt(second * (1.0 / WIDE) - mean * mean + EPS)
    member = []
    for bb in range(2):
        rank_row = rank8[pl.ds(2 * j + bb, 1), :][:, 0:HALO]
        which = hot(rank_row == iota((RT, HALO), 0).astype(F32))
        match = hot(rcv[pl.ds(2 * j + bb, 1), :] == iota((HALO, TILE), 0))
        member.append(dot(which, match).astype(BF))
    for n in range(4):
        cols = slice(n * FEAT, (n + 1) * FEAT)
        old = xe[:, cols].astype(F32)
        fresh = (acc[:, cols] - mean) * scale * gain[0][:, cols] + gain[1][:, cols]
        fresh = jnp.where(both >= 0, old + fresh, old).astype(BF)
        outb[:, cols] = fresh
        for bb in range(2):
            part = dot(member[bb], fresh[bb * TILE : (bb + 1) * TILE, :])
            tsb[bb * RT : (bb + 1) * RT, cols] = part.astype(BF)

    phase("esend")
    my_sums = pl.ds(aligned(j * 2 * RT, 2 * RT), 2 * RT)

    def cols_of(dy):
        return pl.ds(aligned(pairs[dy] * FEAT, FEAT), FEAT)

    sums = start([
        rem(
            tsb.at[:, cols_of(dy)], tsr.at[my_sums], tss.at[dy - 1], tsrr.at[dy - 1],
            (me, pairs[dy]),
        )
        for dy in (2, 1, 3)
    ])
    tsr[my_sums, :] = tsb[:, my_cols]
    phase("n36")
    x_to_z(3)
    phase("n48")
    wy_to_x(4)
    wy_to_x(8)
    phase("w_sums")
    landed(sums)
    phase("sumsend")
    sv[...] = dot(putm[...], tsr[...]).astype(BF)
    my_slot = pl.ds(aligned(me * RT, RT), RT)

    def send_sum(m, t, to):
        rem(sv.at[pl.ds(aligned(to * RT, RT), RT)], vv.at[my_slot], v2s, v2r, (to, j)).start()

    each_patch(send_sum)
    vv[my_slot, :] = sv[my_slot, :]

    order = (2, 1, 3, 0)
    half_n = NROW // 2

    def tables():
        all_ids = pltpu.make_async_copy(idr.at[pl.ds(0, 63)], idr.at[pl.ds(0, 63)], ids_r)
        all_ids.wait()
        ids = idr[:, 0, :]
        bits = [jnp.zeros((PATCH, 1), I32) for _ in range(2)]
        for b in range(BLK):
            held = ids[:, b * 16 : b * 16 + 1] == me
            for k in range(2):
                bits[k] = jnp.where(held, ids[:, b * 16 + 1 + k : b * 16 + 2 + k], bits[k])
        lane2 = iota((PATCH, 128), 1)
        seen = jnp.where(lane2 < 16, bits[0], bits[1])
        seen = lax.shift_right_logical(seen + jnp.zeros_like(lane2), lax.rem(lane2, 16))
        seen = jnp.where(lane2 < HALO, lax.rem(seen, 2), 0)
        rank = jnp.where(seen > 0, dot(seen.astype(F32).astype(BF), low_tri), -1.0)
        listed = jnp.concatenate([hal[...], jnp.zeros((HALO, PATCH), I32)], axis=1)
        listed = jnp.concatenate([listed, jnp.zeros((128 - HALO, 128), I32)], axis=0)
        listed = listed.T[0:PATCH].astype(F32) + 1.0
        wide = iota((PATCH, PATCH * RT), 1)
        mine = wide // RT == iota((PATCH, PATCH * RT), 0)
        spread = jnp.zeros((PATCH, PATCH * RT), F32)
        for r in range(RT):
            node_r = jnp.sum(jnp.where(rank == float(r), listed, 0.0), axis=1, keepdims=True)
            spread = jnp.where(mine & (lax.rem(wide, RT) == r), node_r, spread)
        node_of = jnp.sum(spread, axis=0, keepdims=True).astype(I32) - 1
        for h in range(2):
            for i, dy in enumerate(order):
                low = (4 * h + i) * half_n
                node = iota((half_n, PATCH * RT), 0) + (pairs[dy] * NROW + h * half_n)
                amat[low : low + half_n, :] = hot(node == node_of)

    phase("w_ny")
    phase("eout")
    nodes_in = start([
        rem(
            nl.at[pl.ds(aligned(pairs[dy] * NROW, NROW), NROW)], xn.at[:, my_cols],
            xns.at[dy - 1], xnr.at[dy - 1], (me, pairs[dy]),
        )
        for dy in (2, 1, 3)
    ])
    edges_out = start([
        rem(
            outb.at[:, cols_of(dy)], o_e.at[my_edges], oes.at[dy - 1], oer.at[dy - 1],
            (me, pairs[dy]),
        )
        for dy in (2, 1, 3)
    ])
    o_e[my_edges, :] = outb[:, my_cols]
    phase("w_n3")
    z_to_d(3)
    phase("w_n6")
    z_to_d(6)
    phase("w_ids")
    tables()
    phase("w_nx")
    x_to_z(4)
    x_to_z(8)
    phase("w_nz")
    z_to_d(4)
    z_to_d(8)
    phase("w_nin")
    landed(nodes_in)
    phase("w_nd")
    for u in (3, 4, 6, 8):
        landed(wd[u])
    phase("node1")
    for jr in range(4):
        acc2[:, jr * FEAT : (jr + 1) * FEAT] = dot(xn[...], wa[jr, 3]) + vec[pairs[jr], 3:4, :]

    phase("w_vv")
    got = vv.at[pl.ds(0, 63 * RT)]
    pltpu.make_async_copy(got, got, v2r).wait()
    phase("agg")
    agg_in = []
    for h in range(2):
        rows = slice(h * half_n, (h + 1) * half_n)
        parts = dot(amat[4 * h * half_n : 4 * (h + 1) * half_n, :], vv[...]).astype(BF)
        for i, dy in enumerate(order):
            part = parts[i * half_n : (i + 1) * half_n, :]
            if dy == 0:
                xa[rows, my_cols] = part
            else:
                abuf[dy - 1, rows, :] = part
                agg_in.append(rem(
                    abuf.at[dy - 1, rows], xa.at[rows, my_cols], as_.at[h, dy - 1],
                    ar_.at[h, dy - 1], (me, pairs[dy]),
                ))
                start(agg_in[-1:])
    nodes_out = []
    for h in range(2):
        phase("w_agg%d" % h)
        landed(agg_in[3 * h : 3 * h + 3])
        phase("node2_%d" % h)
        rows = slice(h * half_n, (h + 1) * half_n)
        mixed = None
        for jr in range(4):
            cols = slice(jr * FEAT, (jr + 1) * FEAT)
            hidden = silu(acc2[rows, cols] + dot(xa[rows, :], wa[jr, 4])).astype(BF)
            term = dot(hidden, wb[jr, 1]).astype(BF).astype(F32)
            mixed = term if mixed is None else mixed + term
        old = xn[rows, :].astype(F32)
        live = iota((half_n, 1), 0) + (j * NROW + h * half_n) < cnt[0]
        outn[rows, :] = jnp.where(live, old + norm(mixed, gain[2], gain[3]), old).astype(BF)
        to_rows = pl.ds(aligned(j * NROW + h * half_n, half_n), half_n)
        nodes_out.extend(start([
            rem(
                outn.at[rows, cols_of(dy)], o_n.at[to_rows], ons.at[h, dy - 1], onr.at[h, dy - 1],
                (me, pairs[dy]),
            )
            for dy in (2, 1, 3)
        ]))
        o_n[to_rows, :] = outn[rows, my_cols]

    phase("end_s")
    done = picked.at[pl.ds(0, 63 * HALO)]
    pltpu.make_async_copy(done, done, hs).wait()
    pltpu.make_async_copy(idr.at[pl.ds(0, 63)], idr.at[pl.ds(0, 63)], ids_s).wait()
    pltpu.make_async_copy(got, got, v2s).wait()
    for copy in sent:
        copy.wait_send()
    phase("end_e")
    landed(edges_out)
    phase("end_n")
    landed(nodes_out)
    phase(None)


def shards(
    node_latents, edge_latents, edge_sender, edge_receiver, block_owner, node_counts, halo_nodes,
    w_endpoints, w_edge_in, edge_bias, w_edge_out, edge_gain, edge_shift, w_node_in, node_bias,
    w_node_out, node_gain, node_shift,
):
    row = lambda v: v.reshape(1, FEAT)
    dma = pltpu.SemaphoreType.DMA
    vm = pltpu.VMEM
    scratch = [
        pltpu.SMEM((BLK,), I32), pltpu.SMEM((1,), I32), vm((BLK, TILE), I32), vm((BLK, TILE), I32), vm((HALO, PATCH), I32),
        vm((NODE, FEAT), BF), vm((EDGE, 1), I32), vm((EDGE, FEAT), BF), vm((EDGE, FEAT), BF),
        vm((4, SEL, 1), I32), vm((BLK, TILE, 1), I32), vm((BLK, 128), I32), vm((1, 128), I32),
        vm((BLK, 128), F32),
        vm((PATCH, 1, 128), I32), vm((4, 8, FEAT), F32), vm((4, SEL, FEAT), F32),
        vm((3, SEL, FEAT), BF), vm((SEL, WIDE), BF), vm((ROWS, WIDE), BF), vm((NROW, WIDE), BF),
        vm((4, 5, WIDE, FEAT), BF), vm((4, 2, FEAT, WIDE), BF), vm((WIDE, 2, FEAT), BF),
        vm((ROWS, WIDE), F32), vm((ROWS, WIDE), BF), vm((ROWS, WIDE), BF), vm((2 * RT, WIDE), BF),
        vm((BLK * RT, FEAT), BF), vm((PATCH * RT, FEAT), BF), vm((PATCH * RT, FEAT), BF),
        vm((NODE, PATCH * RT), BF), vm((PATCH * RT, BLK * RT), BF), vm((3, NROW, FEAT), BF),
        vm((NROW, WIDE), BF), vm((NROW, WIDE), F32), vm((NROW, WIDE), BF),
        dma((22,)), dma, dma((4,)), dma, dma, dma((3,)), dma((3,)), dma((3,)), dma((3,)),
        dma((3,)), dma((3,)), dma((9, 3)), dma((9, 3)), dma((9, 2)), dma((9, 2)), dma((9, 2)),
        dma((9, 2)), dma((2, 7)), dma((2, 7)), dma((9,)), dma((9,)), dma((2, 3)), dma((2, 3)), dma((3,)), dma((3,)), dma,
        dma, dma((2, 3)), dma((2, 3)), dma((3,)), dma((3,)), dma((2, 3)), dma((2, 3)),
    ]
    return pl.pallas_call(
        kernel,
        out_shape=(
            vm((NODE, FEAT), BF),
            vm((EDGE, FEAT), BF),
        ),
        in_specs=[ANY] * 18,
        out_specs=(VM, VM),
        scratch_shapes=scratch,
        compiler_params=pltpu.CompilerParams(
            collective_id=0, has_side_effects=True, vmem_limit_bytes=60 * 2**20
        ),
        name="layer",
    )(
        node_latents, edge_latents, edge_sender, edge_receiver, block_owner, node_counts,
        halo_nodes[0].T, w_endpoints, w_edge_in, row(edge_bias), w_edge_out,
        row(edge_gain), row(edge_shift), w_node_in, row(node_bias), w_node_out, row(node_gain),
        row(node_shift),
    )


def solution(mesh):
    return jax.shard_map(
        shards,
        mesh=mesh,
        in_specs=(
            P("patch", "pair"),
            P("patch", "pair"),
            P("patch", None),
            P("patch", None),
            P("patch"),
            P("patch"),
            P("patch", None, None),
            P(None, None, "pair"),
            P(None, "pair"),
            P("pair"),
            P("pair", None),
            P("pair"),
            P("pair"),
            P(None, None, "pair"),
            P("pair"),
            P("pair", None),
            P("pair"),
            P("pair"),
        ),
        out_specs=(P("patch", "pair"), P("patch", "pair")),
        check_vma=False,
    )
```

```python
import jax
import jax.numpy as jnp
from jax import lax
from jax.experimental import pallas as pl
from jax.experimental.pallas import tpu as pltpu
from jax.sharding import PartitionSpec as P

EPS = 1e-05
MESH = pl.DeviceIdType.MESH
BF = jnp.bfloat16
F32 = jnp.float32
I32 = jnp.int32

NODE = 1024
EDGE = 2048
FEAT = 256
WIDE = 1024
PATCH = 64
HALO = 32
RT = 16
BLK = 8
TILE = 256
ROWS = 2 * TILE
SEL = ROWS + 2 * HALO
NROW = NODE // 4
PICK = 2
CUT = 512
ANY = pl.BlockSpec(memory_space=pl.ANY)
VM = pl.BlockSpec(memory_space=pltpu.VMEM)


def iota(shape, dim):
    return lax.broadcasted_iota(I32, shape, dim)


def hot(mask):
    return jnp.where(mask, 1.0, 0.0).astype(BF)


def dot(a, b):
    return jnp.dot(a, b, preferred_element_type=F32)


def silu(v):
    return v / (1.0 + jnp.exp(-v))


def aligned(v, n):
    return pl.multiple_of(v, n)


def kernel(
    nl, el, snd_h, rcv_h, own_h, cnt_h, hal_h, wep, win, eb, wout, eg, es, wnin, nb, wnout, ng, ns,
    o_n, o_e,
    own, cnt, snd, rcv, hal, nl_v, pcol, picked, halo_r, idcol, rcol, idt, idm, rank8, idr, vec, gacc, sbuf, xs,
    xe, xn, wa, wb, wraw, acc, hid, outb, tsb, tsr, sv, vv, amat, putm, abuf, xa, acc2, outn,
    loc, hs, hr, ids_s, ids_r, es_, er_, xns, xnr, vs, vr,
    wys, wyr, wxs, wxr, wzs, wzr, wrs, wrr, wds, wdr, ss, sr, tss, tsrr, v2s, v2r, as_, ar_, oes, oer,
    ons, onr,
):
    me = lax.axis_index("patch")
    j = lax.axis_index("pair")
    z, x, c = lax.div(me, 8), lax.rem(lax.div(me, 2), 4), lax.rem(me, 2)
    cell = [
        lax.rem(x + t // 2, 4) * 2 + lax.rem(c + t % 2, 2) for t in range(8)
    ]

    def dz_of(m):
        odd = lax.rem(m, 2)
        return lax.rem(odd * lax.div(m + 1, 2) + (1 - odd) * (8 - lax.div(m, 2)), 8)

    def plane_of(m):
        return lax.rem(z + dz_of(m), 8) * 8

    def rem(src, dst, s, r, dev):
        return pltpu.make_async_remote_copy(
            src_ref=src, dst_ref=dst, send_sem=s, recv_sem=r, device_id=dev, device_id_type=MESH
        )

    def each_patch(act):
        def plane(m, first):
            base = plane_of(m)
            for t in range(first, 8):
                act(m, t, base + cell[t])

        def step(m, carry):
            plane(m, 0)
            return carry

        plane(0, 1)
        lax.fori_loop(1, 8, step, 0)

    pairs = [lax.rem(j + dy, 4) for dy in range(4)]

    scope = []

    def phase(name):
        if scope:
            scope.pop().__exit__(None, None, None)
        if name:
            scope.append(jax.named_scope(name))
            scope[-1].__enter__()

    phase("start")
    loads = []

    def load(src, dst):
        copy = pltpu.make_async_copy(src, dst, loc.at[len(loads)])
        copy.start()
        loads.append(copy)
        return copy

    my_cols = pl.ds(aligned(j * FEAT, FEAT), FEAT)
    my_edges = pl.ds(aligned(j * ROWS, ROWS), ROWS)
    my_nodes = pl.ds(aligned(j * NROW, NROW), NROW)
    ld_hal = load(hal_h, hal)
    ld_nl = load(nl, nl_v)

    barrier = pltpu.get_barrier_semaphore()

    def greet(m, t, to):
        pl.semaphore_signal(barrier, inc=1, device_id=(to, j), device_id_type=MESH)

    def greet_plane(m, carry):
        base = plane_of(7 - m)
        for t in range(8):
            greet(7 - m, t, base + cell[t])
        return carry

    for dy in (2, 1, 3):
        pl.semaphore_signal(barrier, inc=1, device_id=(me, pairs[dy]), device_id_type=MESH)
    lax.fori_loop(0, 7, greet_plane, 0)
    for t in range(1, 8):
        greet(0, t, plane_of(0) + cell[t])
    ld_e = [load(win, wa.at[0, 0]), load(wep, wraw), load(wout, wb.at[0, 0])]
    ld_i = [load(snd_h, snd), load(rcv_h, rcv), load(own_h, own), load(cnt_h, cnt)]
    ld_i += [
        load(ref, vec.at[j, pl.ds(i, 1)]) for i, ref in enumerate((eb, eg, es, nb, ng, ns))
    ]
    ld_x = [load(el.at[my_edges], xe.at[:, my_cols]), load(nl.at[my_nodes], xn.at[:, my_cols])]
    ld_n = [load(wnin.at[0], wa.at[0, 3]), load(wnin.at[1], wa.at[0, 4]), load(wnout, wb.at[0, 1])]

    phase("cols")
    ld_hal.wait()
    for d in range(PATCH):
        pcol[d * HALO : (d + 1) * HALO, :] = hal[0:HALO, d : d + 1]
    ld_nl.wait()
    phase("pick")

    for m in range(0, 8, PICK):
        wanted = [pcol[pl.ds(aligned(plane_of(m + i) * HALO, 256), 256), :] for i in range(PICK)]
        ones = hot(jnp.concatenate(wanted, axis=0) == iota((PICK * 256, NODE), 1))
        picked[m * 256 : (m + PICK) * 256, :] = dot(ones, nl_v[...]).astype(BF)

    phase("wep")
    piece = c * 4 + x
    for copy in ld_e:
        copy.wait()
    my_rows = pl.ds(aligned(piece * 128, 128), 128)
    wa[0, 1, my_rows, :] = wraw[my_rows, 0, :]
    wa[0, 2, my_rows, :] = wraw[my_rows, 1, :]

    phase("barrier")
    pl.semaphore_wait(barrier, PATCH - 1 + 3)
    phase("sends")

    sent = []

    def start(copies):
        for copy in copies:
            copy.start()
        sent.extend(copies)
        return copies

    def landed(copies):
        for copy in copies:
            copy.wait_recv()

    def seg(u, js, base, low, size):
        if u < 5:
            return wa.at[js, u, pl.ds(aligned(base * 128 + low * 64, 64), size * 64)]
        rows = pl.ds(aligned(base * 32 + low * 16, 16), size * 16)
        cols = pl.ds(0, CUT) if u < 7 else pl.ds(CUT, WIDE - CUT)
        return wb.at[js, (u + 1) % 2, rows, cols]

    def thin(u, js):
        rows = pl.ds(aligned((c * 8 + z) * 16, 16), 16)
        return wb.at[js, (u + 1) % 2, rows, pl.ds(0, CUT)]

    others = pl.ds(1, 3)

    def weights_y(u):
        return start([
            rem(
                thin(u, 0) if u in (5, 6) else seg(u, 0, piece, 0, 2),
                thin(u, 4 - dy) if u in (5, 6) else seg(u, 4 - dy, piece, 0, 2),
                wys.at[u, dy - 1], wyr.at[u, dy - 1], (me, pairs[dy]),
            )
            for dy in (2, 1, 3)
        ])

    right = z * 8 + lax.rem(x + 1, 4) * 2 + c
    left = z * 8 + lax.rem(x + 3, 4) * 2 + c

    def weights_x(u):
        part = seg(u, others, piece, 0, 2)
        return start([
            rem(part, part, wxs.at[u, i], wxr.at[u, i], (to, j)) for i, to in ((0, right), (1, left))
        ])

    def weights_z(u):
        from_left = seg(u, others, c * 4 + lax.rem(x + 3, 4), 0, 1)
        from_right = seg(u, others, c * 4 + lax.rem(x + 1, 4), 1, 1)
        return start([
            rem(from_left, from_left, wzs.at[u, 0], wzr.at[u, 0], (right, j)),
            rem(from_right, from_right, wzs.at[u, 1], wzr.at[u, 1], (left, j)),
        ])

    def weights_round(u):
        return start([
            rem(
                thin(u, others), thin(u, others), wrs.at[u - 5, dz - 1], wrr.at[u - 5, dz - 1],
                (lax.rem(z + dz, 8) * 8 + x * 2 + c, j),
            )
            for dz in (4, 3, 5, 2, 6, 1, 7)
        ])

    def weights_d(u):
        part = seg(u, others, c * 4, 0, 8)
        return start([rem(part, part, wds.at[u], wdr.at[u], (z * 8 + x * 2 + 1 - c, j))])

    def send_halo(m, t, to):
        rem(
            picked.at[pl.ds(aligned(m * 256 + cell[t] * HALO, HALO), HALO)],
            halo_r.at[pl.ds(aligned((m * 8 + t) * HALO, HALO), HALO)],
            hs, hr.at[lax.div(m, 2)], (to, j),
        ).start()

    order_e = (0, 1, 2, 7, 5)
    wy = {0: weights_y(0)}
    each_patch(send_halo)
    halo_r[0:HALO, :] = picked[pl.ds(aligned(cell[0] * HALO, HALO), HALO), :]
    wx, wz, wd = {}, {}, {}

    part_a, part_b = slice(0, TILE + 2 * HALO), slice(TILE + 2 * HALO, SEL)

    def gather(g):
        slot = g * 16 + iota((1, 512), 1) // HALO
        m = slot // 8
        odd = lax.rem(m, 2)
        dz = odd * ((m + 1) // 2) + (1 - odd) * (8 - m // 2)
        t = lax.rem(slot, 8)
        source = (
            lax.rem(z - dz + 16, 8) * 8 + lax.rem(x - t // 2 + 4, 4) * 2
            + lax.rem(c + lax.rem(t, 2), 2)
        )
        ident = source * HALO + lax.rem(iota((1, 512), 1), HALO)
        low = HALO if g == 0 else 0
        arrived = halo_r.at[pl.ds(g * 512 + low, 512 - low)]
        pltpu.make_async_copy(arrived, arrived, hr.at[g]).wait()
        if g == 3:
            wz[5] = weights_round(5)
        table = halo_r.at[g * 512 : (g + 1) * 512]
        if g < 3:
            for dy in (2, 1, 3, 0):
                part = dot(hot(idcol[pairs[dy]] == ident), table[...])
                gacc[dy] = part if g == 0 else gacc[dy] + part
            return []
        copies = []
        for half, rows in enumerate((part_a, part_b)):
            for dy in (2, 1, 3, 0):
                part = dot(hot(idcol[pairs[dy], rows, :] == ident), table[...])
                part = (gacc[dy, rows, :] + part).astype(BF)
                if dy == 0:
                    xs[rows, my_cols] = part
                else:
                    sbuf[dy - 1, rows, :] = part
                    copies.append(rem(
                        sbuf.at[dy - 1, rows], xs.at[rows, my_cols], ss.at[half, dy - 1],
                        sr.at[half, dy - 1], (me, pairs[dy]),
                    ))
                    start(copies[-1:])
        return copies

    def wy_to_x(u):
        landed(wy[u])
        wx[u] = weights_x(u)

    def x_to_z(u):
        landed(wx[u])
        wz[u] = weights_z(u)

    def z_to_d(u):
        landed(wz[u])
        wd[u] = weights_d(u)

    def block_ids():
        snd_t = snd[...].T
        rcv_t = rcv[...].T
        lane = iota((TILE, 128), 1)
        for b in range(BLK):
            g, low = b // 2, 2 * HALO + (b % 2) * TILE
            idcol[g, low : low + TILE, :] = snd_t[:, b : b + 1]
            low = (b % 2) * HALO
            idcol[g, low : low + HALO, :] = iota((HALO, 1), 0) + own[b] * HALO
            rcol[b] = rcv_t[:, b : b + 1]
            seen = jnp.max(jnp.where(rcv_t[:, b : b + 1] == lane, 1, 0), axis=0, keepdims=True)
            idt[b : b + 1, :] = seen

    phase("idcols")
    for copy in ld_i:
        copy.wait()
    block_ids()
    phase("vecs")
    for u in order_e[1:]:
        wy[u] = weights_y(u)
    vecs = start([
        rem(vec.at[j], vec.at[j], vs.at[dy - 1], vr.at[dy - 1], (me, pairs[dy]))
        for dy in (2, 1, 3)
    ])

    phase("wy0")
    wy_to_x(0)
    phase("wep2")

    def split(k, carry):
        rows = pl.ds(aligned(lax.rem(piece + k, 8) * 128, 128), 128)
        wa[0, 1, rows, :] = wraw[rows, 0, :]
        wa[0, 2, rows, :] = wraw[rows, 1, :]
        return carry

    lax.fori_loop(1, 8, split, 0)
    phase("edgesin")
    edges_in = start([
        rem(
            el.at[pl.ds(aligned(pairs[dy] * ROWS, ROWS), ROWS)], xe.at[:, my_cols],
            es_.at[dy - 1], er_.at[dy - 1], (me, pairs[dy]),
        )
        for dy in (2, 1, 3)
    ])
    phase("g0")
    gather(0)
    phase("wy1")
    wy_to_x(1)
    phase("wy2")
    wy_to_x(2)
    for copy in ld_n:
        copy.wait()
    for u in (3, 6):
        wy[u] = weights_y(u)
    phase("g1")
    gather(1)
    phase("wy5")
    landed(wy[5])
    wy_to_x(7)
    phase("x0")
    x_to_z(0)
    phase("g2")
    gather(2)
    phase("ny")
    phase("x1")
    x_to_z(1)
    phase("g3")
    rows_in = gather(3)
    phase("ldn")
    for copy in ld_x:
        copy.wait()
    phase("z0")
    z_to_d(0)
    phase("x2")
    x_to_z(2)
    phase("x7")
    x_to_z(7)
    phase("z1")
    z_to_d(1)

    phase("tables")
    low_tri = hot(iota((128, 128), 0) < iota((128, 128), 1))
    live8 = jnp.where(iota((BLK, 128), 1) < HALO, idt[...], 0)
    lane8 = iota((BLK, 128), 1)
    bit = lax.shift_left(jnp.ones((BLK, 128), I32), lax.rem(lane8, 16))
    bits = [
        jnp.sum(jnp.where(lane8 // 16 == k, live8 * bit, 0), axis=1, keepdims=True) for k in range(2)
    ]
    lane1 = iota((1, 128), 1)
    message = jnp.zeros((1, 128), I32)
    for b in range(BLK):
        message = jnp.where(lane1 == b * 16, own[b], message)
        for k in range(2):
            message = jnp.where(lane1 == b * 16 + 1 + k, bits[k][b : b + 1, :], message)
    idm[...] = message
    def send_ids(m, t, to):
        rem(idm, idr.at[me], ids_s, ids_r, (to, j)).start()

    each_patch(send_ids)
    idr[me] = idm[...]

    rank8[...] = jnp.where(live8 > 0, dot(live8.astype(F32).astype(BF), low_tri), -1.0)
    wide_k = iota((1, BLK * RT), 1)
    owner_row = jnp.zeros((1, BLK * RT), I32)
    for b in range(BLK):
        owner_row = jnp.where(wide_k // RT == b, own[b], owner_row)
    rid = iota((PATCH * RT, BLK * RT), 0)
    putm[...] = hot((rid // RT == owner_row) & (lax.rem(rid, RT) == lax.rem(wide_k, RT)))

    phase("z2")
    z_to_d(2)
    phase("z5w")
    landed(wz[5])
    wd[5] = weights_d(5)
    phase("w_edges")
    landed(edges_in)
    landed(vecs)
    phase("w_d0")
    landed(wd[0])
    phase("edge1")
    for jr in range(4):
        acc[:, jr * FEAT : (jr + 1) * FEAT] = dot(xe[...], wa[jr, 0]) + vec[pairs[jr], 0:1, :]
    gain = [jnp.concatenate([vec[k, i : i + 1, :] for k in range(4)], axis=1) for i in (1, 2, 4, 5)]
    phase("z7")
    z_to_d(7)
    phase("n3")
    landed(wy[6])
    wz[6] = weights_round(6)
    wy_to_x(3)
    phase("w_rows0")
    landed(rows_in[0:3])
    phase("w_d")
    landed(wd[1])
    landed(wd[2])
    landed(wd[5])
    landed(wd[7])

    def norm(mixed, gain_row, shift_row):
        mean = jnp.sum(mixed, axis=1, keepdims=True) * (1.0 / WIDE)
        spread = jnp.sum(mixed * mixed, axis=1, keepdims=True) * (1.0 / WIDE) - mean * mean
        return (mixed - mean) * lax.rsqrt(spread + EPS) * gain_row + shift_row

    phase("section")
    section = [dot(xs[0 : 2 * HALO, :], wa[k, 2]).astype(BF) for k in range(4)]
    phase("w_rows1")
    both = jnp.concatenate([rcol[2 * j], rcol[2 * j + 1]], axis=0)
    lane2 = iota((ROWS, 2 * HALO), 1)
    base2 = (iota((ROWS, 2 * HALO), 0) // TILE) * HALO
    take = hot((both >= 0) & (both + base2 == lane2))
    landed(rows_in[3:6])
    for u in (4, 8):
        wy[u] = weights_y(u)
    phase("edge2a")
    for k in range(4):
        cols = slice(k * FEAT, (k + 1) * FEAT)
        pre = acc[:, cols] + dot(xs[2 * HALO :, :], wa[k, 1]) + dot(take, section[k])
        hid[:, cols] = silu(pre).astype(BF)
    phase("x346")
    phase("edge2b")
    first = jnp.zeros((ROWS, 1), F32)
    second = jnp.zeros((ROWS, 1), F32)
    for n in range(4):
        cols = slice(n * FEAT, (n + 1) * FEAT)
        mixed = None
        for k in range(4):
            term = dot(hid[:, k * FEAT : (k + 1) * FEAT], wb[k, 0, :, cols]).astype(BF).astype(F32)
            mixed = term if mixed is None else mixed + term
        acc[:, cols] = mixed
        first = first + jnp.sum(mixed, axis=1, keepdims=True)
        second = second + jnp.sum(mixed * mixed, axis=1, keepdims=True)
    mean = first * (1.0 / WIDE)
    scale = lax.rsqrt(second * (1.0 / WIDE) - mean * mean + EPS)
    member = []
    for bb in range(2):
        rank_row = rank8[pl.ds(2 * j + bb, 1), :][:, 0:HALO]
        which = hot(rank_row == iota((RT, HALO), 0).astype(F32))
        match = hot(rcv[pl.ds(2 * j + bb, 1), :] == iota((HALO, TILE), 0))
        member.append(dot(which, match).astype(BF))
    for n in range(4):
        cols = slice(n * FEAT, (n + 1) * FEAT)
        old = xe[:, cols].astype(F32)
        fresh = (acc[:, cols] - mean) * scale * gain[0][:, cols] + gain[1][:, cols]
        fresh = jnp.where(both >= 0, old + fresh, old).astype(BF)
        outb[:, cols] = fresh
        for bb in range(2):
            part = dot(member[bb], fresh[bb * TILE : (bb + 1) * TILE, :])
            tsb[bb * RT : (bb + 1) * RT, cols] = part.astype(BF)

    phase("esend")
    my_sums = pl.ds(aligned(j * 2 * RT, 2 * RT), 2 * RT)

    def cols_of(dy):
        return pl.ds(aligned(pairs[dy] * FEAT, FEAT), FEAT)

    sums = start([
        rem(
            tsb.at[:, cols_of(dy)], tsr.at[my_sums], tss.at[dy - 1], tsrr.at[dy - 1],
            (me, pairs[dy]),
        )
        for dy in (2, 1, 3)
    ])
    tsr[my_sums, :] = tsb[:, my_cols]
    phase("n36")
    x_to_z(3)
    phase("n48")
    wy_to_x(4)
    wy_to_x(8)
    nodes_in = start([
        rem(
            nl.at[pl.ds(aligned(pairs[dy] * NROW, NROW), NROW)], xn.at[:, my_cols],
            xns.at[dy - 1], xnr.at[dy - 1], (me, pairs[dy]),
        )
        for dy in (2, 1, 3)
    ])
    edges_out = start([
        rem(
            outb.at[:, cols_of(dy)], o_e.at[my_edges], oes.at[dy - 1], oer.at[dy - 1],
            (me, pairs[dy]),
        )
        for dy in (2, 1, 3)
    ])
    phase("w_sums")
    landed(sums)
    phase("sumsend")
    sv[...] = dot(putm[...], tsr[...]).astype(BF)
    my_slot = pl.ds(aligned(me * RT, RT), RT)

    def send_sum(m, t, to):
        rem(sv.at[pl.ds(aligned(to * RT, RT), RT)], vv.at[my_slot], v2s, v2r, (to, j)).start()

    each_patch(send_sum)
    vv[my_slot, :] = sv[my_slot, :]

    order = (2, 1, 3, 0)
    half_n = NROW // 2

    def tables():
        all_ids = pltpu.make_async_copy(idr.at[pl.ds(0, 63)], idr.at[pl.ds(0, 63)], ids_r)
        all_ids.wait()
        ids = idr[:, 0, :]
        bits = [jnp.zeros((PATCH, 1), I32) for _ in range(2)]
        for b in range(BLK):
            held = ids[:, b * 16 : b * 16 + 1] == me
            for k in range(2):
                bits[k] = jnp.where(held, ids[:, b * 16 + 1 + k : b * 16 + 2 + k], bits[k])
        lane2 = iota((PATCH, 128), 1)
        seen = jnp.where(lane2 < 16, bits[0], bits[1])
        seen = lax.shift_right_logical(seen + jnp.zeros_like(lane2), lax.rem(lane2, 16))
        seen = jnp.where(lane2 < HALO, lax.rem(seen, 2), 0)
        rank = jnp.where(seen > 0, dot(seen.astype(F32).astype(BF), low_tri), -1.0)
        listed = jnp.concatenate([hal[...], jnp.zeros((HALO, PATCH), I32)], axis=1)
        listed = jnp.concatenate([listed, jnp.zeros((128 - HALO, 128), I32)], axis=0)
        listed = listed.T[0:PATCH].astype(F32) + 1.0
        wide = iota((PATCH, PATCH * RT), 1)
        mine = wide // RT == iota((PATCH, PATCH * RT), 0)
        spread = jnp.zeros((PATCH, PATCH * RT), F32)
        for r in range(RT):
            node_r = jnp.sum(jnp.where(rank == float(r), listed, 0.0), axis=1, keepdims=True)
            spread = jnp.where(mine & (lax.rem(wide, RT) == r), node_r, spread)
        node_of = jnp.sum(spread, axis=0, keepdims=True).astype(I32) - 1
        for h in range(2):
            for i, dy in enumerate(order):
                low = (4 * h + i) * half_n
                node = iota((half_n, PATCH * RT), 0) + (pairs[dy] * NROW + h * half_n)
                amat[low : low + half_n, :] = hot(node == node_of)

    phase("w_ny")
    phase("eout")
    o_e[my_edges, :] = outb[:, my_cols]
    phase("w_n3")
    z_to_d(3)
    phase("w_n6")
    z_to_d(6)
    phase("w_ids")
    tables()
    phase("w_nx")
    x_to_z(4)
    x_to_z(8)
    phase("w_nin")
    landed(nodes_in)
    phase("w_nd")
    landed(wd[3])
    phase("node1")
    for jr in range(4):
        acc2[:, jr * FEAT : (jr + 1) * FEAT] = dot(xn[...], wa[jr, 3]) + vec[pairs[jr], 3:4, :]

    phase("w_vv")
    got = vv.at[pl.ds(0, 63 * RT)]
    pltpu.make_async_copy(got, got, v2r).wait()
    phase("agg")
    agg_in = []
    for h in range(2):
        rows = slice(h * half_n, (h + 1) * half_n)
        parts = dot(amat[4 * h * half_n : 4 * (h + 1) * half_n, :], vv[...]).astype(BF)
        for i, dy in enumerate(order):
            part = parts[i * half_n : (i + 1) * half_n, :]
            if dy == 0:
                xa[rows, my_cols] = part
            else:
                abuf[dy - 1, rows, :] = part
                agg_in.append(rem(
                    abuf.at[dy - 1, rows], xa.at[rows, my_cols], as_.at[h, dy - 1],
                    ar_.at[h, dy - 1], (me, pairs[dy]),
                ))
                start(agg_in[-1:])
    phase("w_nz")
    z_to_d(4)
    z_to_d(8)
    phase("w_nd2")
    for u in (6, 4, 8):
        landed(wd[u])
    nodes_out = []
    for h in range(2):
        phase("w_agg%d" % h)
        landed(agg_in[3 * h : 3 * h + 3])
        phase("node2_%d" % h)
        rows = slice(h * half_n, (h + 1) * half_n)
        mixed = None
        for jr in range(4):
            cols = slice(jr * FEAT, (jr + 1) * FEAT)
            hidden = silu(acc2[rows, cols] + dot(xa[rows, :], wa[jr, 4])).astype(BF)
            term = dot(hidden, wb[jr, 1]).astype(BF).astype(F32)
            mixed = term if mixed is None else mixed + term
        old = xn[rows, :].astype(F32)
        live = iota((half_n, 1), 0) + (j * NROW + h * half_n) < cnt[0]
        outn[rows, :] = jnp.where(live, old + norm(mixed, gain[2], gain[3]), old).astype(BF)
        to_rows = pl.ds(aligned(j * NROW + h * half_n, half_n), half_n)
        nodes_out.extend(start([
            rem(
                outn.at[rows, cols_of(dy)], o_n.at[to_rows], ons.at[h, dy - 1], onr.at[h, dy - 1],
                (me, pairs[dy]),
            )
            for dy in (2, 1, 3)
        ]))
        o_n[to_rows, :] = outn[rows, my_cols]

    phase("end_s")
    done = picked.at[pl.ds(0, 63 * HALO)]
    pltpu.make_async_copy(done, done, hs).wait()
    pltpu.make_async_copy(idr.at[pl.ds(0, 63)], idr.at[pl.ds(0, 63)], ids_s).wait()
    pltpu.make_async_copy(got, got, v2s).wait()
    for copy in sent:
        copy.wait_send()
    phase("end_e")
    landed(edges_out)
    phase("end_n")
    landed(nodes_out)
    phase(None)


def shards(
    node_latents, edge_latents, edge_sender, edge_receiver, block_owner, node_counts, halo_nodes,
    w_endpoints, w_edge_in, edge_bias, w_edge_out, edge_gain, edge_shift, w_node_in, node_bias,
    w_node_out, node_gain, node_shift,
):
    row = lambda v: v.reshape(1, FEAT)
    dma = pltpu.SemaphoreType.DMA
    vm = pltpu.VMEM
    scratch = [
        pltpu.SMEM((BLK,), I32), pltpu.SMEM((1,), I32), vm((BLK, TILE), I32), vm((BLK, TILE), I32), vm((HALO, PATCH), I32),
        vm((NODE, FEAT), BF), vm((EDGE, 1), I32), vm((EDGE, FEAT), BF), vm((EDGE, FEAT), BF),
        vm((4, SEL, 1), I32), vm((BLK, TILE, 1), I32), vm((BLK, 128), I32), vm((1, 128), I32),
        vm((BLK, 128), F32),
        vm((PATCH, 1, 128), I32), vm((4, 8, FEAT), F32), vm((4, SEL, FEAT), F32),
        vm((3, SEL, FEAT), BF), vm((SEL, WIDE), BF), vm((ROWS, WIDE), BF), vm((NROW, WIDE), BF),
        vm((4, 5, WIDE, FEAT), BF), vm((4, 2, FEAT, WIDE), BF), vm((WIDE, 2, FEAT), BF),
        vm((ROWS, WIDE), F32), vm((ROWS, WIDE), BF), vm((ROWS, WIDE), BF), vm((2 * RT, WIDE), BF),
        vm((BLK * RT, FEAT), BF), vm((PATCH * RT, FEAT), BF), vm((PATCH * RT, FEAT), BF),
        vm((NODE, PATCH * RT), BF), vm((PATCH * RT, BLK * RT), BF), vm((3, NROW, FEAT), BF),
        vm((NROW, WIDE), BF), vm((NROW, WIDE), F32), vm((NROW, WIDE), BF),
        dma((22,)), dma, dma((4,)), dma, dma, dma((3,)), dma((3,)), dma((3,)), dma((3,)),
        dma((3,)), dma((3,)), dma((9, 3)), dma((9, 3)), dma((9, 2)), dma((9, 2)), dma((9, 2)),
        dma((9, 2)), dma((2, 7)), dma((2, 7)), dma((9,)), dma((9,)), dma((2, 3)), dma((2, 3)), dma((3,)), dma((3,)), dma,
        dma, dma((2, 3)), dma((2, 3)), dma((3,)), dma((3,)), dma((2, 3)), dma((2, 3)),
    ]
    return pl.pallas_call(
        kernel,
        out_shape=(
            vm((NODE, FEAT), BF),
            vm((EDGE, FEAT), BF),
        ),
        in_specs=[ANY] * 18,
        out_specs=(VM, VM),
        scratch_shapes=scratch,
        compiler_params=pltpu.CompilerParams(
            collective_id=0, has_side_effects=True, vmem_limit_bytes=60 * 2**20
        ),
        name="layer",
    )(
        node_latents, edge_latents, edge_sender, edge_receiver, block_owner, node_counts,
        halo_nodes[0].T, w_endpoints, w_edge_in, row(edge_bias), w_edge_out,
        row(edge_gain), row(edge_shift), w_node_in, row(node_bias), w_node_out, row(node_gain),
        row(node_shift),
    )


def solution(mesh):
    return jax.shard_map(
        shards,
        mesh=mesh,
        in_specs=(
            P("patch", "pair"),
            P("patch", "pair"),
            P("patch", None),
            P("patch", None),
            P("patch"),
            P("patch"),
            P("patch", None, None),
            P(None, None, "pair"),
            P(None, "pair"),
            P("pair"),
            P("pair", None),
            P("pair"),
            P("pair"),
            P(None, None, "pair"),
            P("pair"),
            P("pair", None),
            P("pair"),
            P("pair"),
        ),
        out_specs=(P("patch", "pair"), P("patch", "pair")),
        check_vma=False,
    )
```

```python
import jax
import jax.numpy as jnp
from jax import lax
from jax.experimental import pallas as pl
from jax.experimental.pallas import tpu as pltpu
from jax.sharding import PartitionSpec as P

EPS = 1e-05
MESH = pl.DeviceIdType.MESH
BF = jnp.bfloat16
F32 = jnp.float32
I32 = jnp.int32

NODE = 1024
EDGE = 2048
FEAT = 256
WIDE = 1024
PATCH = 64
HALO = 32
RT = 16
BLK = 8
TILE = 256
ROWS = 2 * TILE
SEL = ROWS + 2 * HALO
NROW = NODE // 4
PICK = 2
CUT = (512, 640)
ANY = pl.BlockSpec(memory_space=pl.ANY)
VM = pl.BlockSpec(memory_space=pltpu.VMEM)


def iota(shape, dim):
    return lax.broadcasted_iota(I32, shape, dim)


def hot(mask):
    return jnp.where(mask, 1.0, 0.0).astype(BF)


def dot(a, b):
    return jnp.dot(a, b, preferred_element_type=F32)


def silu(v):
    return v / (1.0 + jnp.exp(-v))


def aligned(v, n):
    return pl.multiple_of(v, n)


def kernel(
    nl, el, snd_h, rcv_h, own_h, cnt_h, hal_h, wep, win, eb, wout, eg, es, wnin, nb, wnout, ng, ns,
    o_n, o_e,
    own, cnt, snd, rcv, hal, nl_v, pcol, picked, halo_r, idcol, rcol, idt, idm, rank8, idr, vec, gacc, sbuf, xs,
    xe, xn, wa, wb, wraw, acc, hid, outb, tsb, tsr, sv, vv, amat, putm, abuf, xa, acc2, outn,
    loc, hs, hr, ids_s, ids_r, es_, er_, xns, xnr, vs, vr,
    wys, wyr, wxs, wxr, wzs, wzr, wrs, wrr, wds, wdr, ss, sr, tss, tsrr, v2s, v2r, as_, ar_, oes, oer,
    ons, onr,
):
    me = lax.axis_index("patch")
    j = lax.axis_index("pair")
    z, x, c = lax.div(me, 8), lax.rem(lax.div(me, 2), 4), lax.rem(me, 2)
    cell = [
        lax.rem(x + t // 2, 4) * 2 + lax.rem(c + t % 2, 2) for t in range(8)
    ]

    def dz_of(m):
        odd = lax.rem(m, 2)
        return lax.rem(odd * lax.div(m + 1, 2) + (1 - odd) * (8 - lax.div(m, 2)), 8)

    def plane_of(m):
        return lax.rem(z + dz_of(m), 8) * 8

    def rem(src, dst, s, r, dev):
        return pltpu.make_async_remote_copy(
            src_ref=src, dst_ref=dst, send_sem=s, recv_sem=r, device_id=dev, device_id_type=MESH
        )

    def each_patch(act):
        def plane(m, first):
            base = plane_of(m)
            for t in range(first, 8):
                act(m, t, base + cell[t])

        def step(m, carry):
            plane(m, 0)
            return carry

        plane(0, 1)
        lax.fori_loop(1, 8, step, 0)

    pairs = [lax.rem(j + dy, 4) for dy in range(4)]

    scope = []

    def phase(name):
        if scope:
            scope.pop().__exit__(None, None, None)
        if name:
            scope.append(jax.named_scope(name))
            scope[-1].__enter__()

    phase("start")
    loads = []

    def load(src, dst):
        copy = pltpu.make_async_copy(src, dst, loc.at[len(loads)])
        copy.start()
        loads.append(copy)
        return copy

    my_cols = pl.ds(aligned(j * FEAT, FEAT), FEAT)
    my_edges = pl.ds(aligned(j * ROWS, ROWS), ROWS)
    my_nodes = pl.ds(aligned(j * NROW, NROW), NROW)
    ld_hal = load(hal_h, hal)
    ld_nl = load(nl, nl_v)

    barrier = pltpu.get_barrier_semaphore()

    def greet(m, t, to):
        pl.semaphore_signal(barrier, inc=1, device_id=(to, j), device_id_type=MESH)

    def greet_plane(m, carry):
        base = plane_of(7 - m)
        for t in range(8):
            greet(7 - m, t, base + cell[t])
        return carry

    for dy in (2, 1, 3):
        pl.semaphore_signal(barrier, inc=1, device_id=(me, pairs[dy]), device_id_type=MESH)
    lax.fori_loop(0, 7, greet_plane, 0)
    for t in range(1, 8):
        greet(0, t, plane_of(0) + cell[t])
    ld_e = [load(win, wa.at[0, 0]), load(wep, wraw), load(wout, wb.at[0, 0])]
    ld_i = [load(snd_h, snd), load(rcv_h, rcv), load(own_h, own), load(cnt_h, cnt)]
    ld_i += [
        load(ref, vec.at[j, pl.ds(i, 1)]) for i, ref in enumerate((eb, eg, es, nb, ng, ns))
    ]
    ld_x = [load(el.at[my_edges], xe.at[:, my_cols]), load(nl.at[my_nodes], xn.at[:, my_cols])]
    ld_n = [load(wnin.at[0], wa.at[0, 3]), load(wnin.at[1], wa.at[0, 4]), load(wnout, wb.at[0, 1])]

    phase("cols")
    ld_hal.wait()
    for d in range(PATCH):
        pcol[d * HALO : (d + 1) * HALO, :] = hal[0:HALO, d : d + 1]
    ld_nl.wait()
    phase("pick")

    for m in range(0, 8, PICK):
        wanted = [pcol[pl.ds(aligned(plane_of(m + i) * HALO, 256), 256), :] for i in range(PICK)]
        ones = hot(jnp.concatenate(wanted, axis=0) == iota((PICK * 256, NODE), 1))
        picked[m * 256 : (m + PICK) * 256, :] = dot(ones, nl_v[...]).astype(BF)

    phase("wep")
    piece = c * 4 + x
    for copy in ld_e:
        copy.wait()
    my_rows = pl.ds(aligned(piece * 128, 128), 128)
    wa[0, 1, my_rows, :] = wraw[my_rows, 0, :]
    wa[0, 2, my_rows, :] = wraw[my_rows, 1, :]

    phase("barrier")
    pl.semaphore_wait(barrier, PATCH - 1 + 3)
    phase("sends")

    sent = []

    def start(copies):
        for copy in copies:
            copy.start()
        sent.extend(copies)
        return copies

    def landed(copies):
        for copy in copies:
            copy.wait_recv()

    def seg(u, js, base, low, size):
        if u < 5:
            return wa.at[js, u, pl.ds(aligned(base * 128 + low * 64, 64), size * 64)]
        rows = pl.ds(aligned(base * 32 + low * 16, 16), size * 16)
        b = (u + 1) % 2
        cols = pl.ds(0, CUT[b]) if u < 7 else pl.ds(CUT[b], WIDE - CUT[b])
        return wb.at[js, b, rows, cols]

    def thin(u, js):
        rows = pl.ds(aligned((c * 8 + z) * 16, 16), 16)
        b = (u + 1) % 2
        return wb.at[js, b, rows, pl.ds(0, CUT[b])]

    others = pl.ds(1, 3)

    def weights_y(u):
        return start([
            rem(
                thin(u, 0) if u in (5, 6) else seg(u, 0, piece, 0, 2),
                thin(u, 4 - dy) if u in (5, 6) else seg(u, 4 - dy, piece, 0, 2),
                wys.at[u, dy - 1], wyr.at[u, dy - 1], (me, pairs[dy]),
            )
            for dy in (2, 1, 3)
        ])

    right = z * 8 + lax.rem(x + 1, 4) * 2 + c
    left = z * 8 + lax.rem(x + 3, 4) * 2 + c

    def weights_x(u):
        part = seg(u, others, piece, 0, 2)
        return start([
            rem(part, part, wxs.at[u, i], wxr.at[u, i], (to, j)) for i, to in ((0, right), (1, left))
        ])

    def weights_z(u):
        from_left = seg(u, others, c * 4 + lax.rem(x + 3, 4), 0, 1)
        from_right = seg(u, others, c * 4 + lax.rem(x + 1, 4), 1, 1)
        return start([
            rem(from_left, from_left, wzs.at[u, 0], wzr.at[u, 0], (right, j)),
            rem(from_right, from_right, wzs.at[u, 1], wzr.at[u, 1], (left, j)),
        ])

    def weights_round(u):
        return start([
            rem(
                thin(u, others), thin(u, others), wrs.at[u - 5, dz - 1], wrr.at[u - 5, dz - 1],
                (lax.rem(z + dz, 8) * 8 + x * 2 + c, j),
            )
            for dz in (4, 3, 5, 2, 6, 1, 7)
        ])

    def weights_d(u):
        part = seg(u, others, c * 4, 0, 8)
        return start([rem(part, part, wds.at[u], wdr.at[u], (z * 8 + x * 2 + 1 - c, j))])

    def send_halo(m, t, to):
        rem(
            picked.at[pl.ds(aligned(m * 256 + cell[t] * HALO, HALO), HALO)],
            halo_r.at[pl.ds(aligned((m * 8 + t) * HALO, HALO), HALO)],
            hs, hr.at[lax.div(m, 2)], (to, j),
        ).start()

    order_e = (0, 1, 2, 7, 5)
    wy = {0: weights_y(0)}
    each_patch(send_halo)
    halo_r[0:HALO, :] = picked[pl.ds(aligned(cell[0] * HALO, HALO), HALO), :]
    wx, wz, wd = {}, {}, {}

    part_a, part_b = slice(0, TILE + 2 * HALO), slice(TILE + 2 * HALO, SEL)

    def gather(g):
        slot = g * 16 + iota((1, 512), 1) // HALO
        m = slot // 8
        odd = lax.rem(m, 2)
        dz = odd * ((m + 1) // 2) + (1 - odd) * (8 - m // 2)
        t = lax.rem(slot, 8)
        source = (
            lax.rem(z - dz + 16, 8) * 8 + lax.rem(x - t // 2 + 4, 4) * 2
            + lax.rem(c + lax.rem(t, 2), 2)
        )
        ident = source * HALO + lax.rem(iota((1, 512), 1), HALO)
        low = HALO if g == 0 else 0
        arrived = halo_r.at[pl.ds(g * 512 + low, 512 - low)]
        pltpu.make_async_copy(arrived, arrived, hr.at[g]).wait()
        if g == 3:
            wz[5] = weights_round(5)
        table = halo_r.at[g * 512 : (g + 1) * 512]
        if g < 3:
            for dy in (2, 1, 3, 0):
                part = dot(hot(idcol[pairs[dy]] == ident), table[...])
                gacc[dy] = part if g == 0 else gacc[dy] + part
            return []
        copies = []
        for half, rows in enumerate((part_a, part_b)):
            for dy in (2, 1, 3, 0):
                part = dot(hot(idcol[pairs[dy], rows, :] == ident), table[...])
                part = (gacc[dy, rows, :] + part).astype(BF)
                if dy == 0:
                    xs[rows, my_cols] = part
                else:
                    sbuf[dy - 1, rows, :] = part
                    copies.append(rem(
                        sbuf.at[dy - 1, rows], xs.at[rows, my_cols], ss.at[half, dy - 1],
                        sr.at[half, dy - 1], (me, pairs[dy]),
                    ))
                    start(copies[-1:])
        return copies

    def wy_to_x(u):
        landed(wy[u])
        wx[u] = weights_x(u)

    def x_to_z(u):
        landed(wx[u])
        wz[u] = weights_z(u)

    def z_to_d(u):
        landed(wz[u])
        wd[u] = weights_d(u)

    def block_ids():
        snd_t = snd[...].T
        rcv_t = rcv[...].T
        lane = iota((TILE, 128), 1)
        for b in range(BLK):
            g, low = b // 2, 2 * HALO + (b % 2) * TILE
            idcol[g, low : low + TILE, :] = snd_t[:, b : b + 1]
            low = (b % 2) * HALO
            idcol[g, low : low + HALO, :] = iota((HALO, 1), 0) + own[b] * HALO
            rcol[b] = rcv_t[:, b : b + 1]
            seen = jnp.max(jnp.where(rcv_t[:, b : b + 1] == lane, 1, 0), axis=0, keepdims=True)
            idt[b : b + 1, :] = seen

    phase("idcols")
    for copy in ld_i:
        copy.wait()
    block_ids()
    phase("vecs")
    for u in order_e[1:]:
        wy[u] = weights_y(u)
    vecs = start([
        rem(vec.at[j], vec.at[j], vs.at[dy - 1], vr.at[dy - 1], (me, pairs[dy]))
        for dy in (2, 1, 3)
    ])

    phase("wy0")
    wy_to_x(0)
    phase("wep2")

    def split(k, carry):
        rows = pl.ds(aligned(lax.rem(piece + k, 8) * 128, 128), 128)
        wa[0, 1, rows, :] = wraw[rows, 0, :]
        wa[0, 2, rows, :] = wraw[rows, 1, :]
        return carry

    lax.fori_loop(1, 8, split, 0)
    phase("edgesin")
    edges_in = start([
        rem(
            el.at[pl.ds(aligned(pairs[dy] * ROWS, ROWS), ROWS)], xe.at[:, my_cols],
            es_.at[dy - 1], er_.at[dy - 1], (me, pairs[dy]),
        )
        for dy in (2, 1, 3)
    ])
    phase("g0")
    gather(0)
    phase("wy1")
    wy_to_x(1)
    phase("wy2")
    wy_to_x(2)
    for copy in ld_n:
        copy.wait()
    for u in (3, 6):
        wy[u] = weights_y(u)
    phase("g1")
    gather(1)
    phase("wy5")
    landed(wy[5])
    wy_to_x(7)
    phase("x0")
    x_to_z(0)
    phase("g2")
    gather(2)
    phase("ny")
    phase("x1")
    x_to_z(1)
    phase("g3")
    rows_in = gather(3)
    phase("ldn")
    for copy in ld_x:
        copy.wait()
    phase("z0")
    z_to_d(0)
    phase("x2")
    x_to_z(2)
    phase("x7")
    x_to_z(7)
    phase("z1")
    z_to_d(1)

    phase("tables")
    low_tri = hot(iota((128, 128), 0) < iota((128, 128), 1))
    live8 = jnp.where(iota((BLK, 128), 1) < HALO, idt[...], 0)
    lane8 = iota((BLK, 128), 1)
    bit = lax.shift_left(jnp.ones((BLK, 128), I32), lax.rem(lane8, 16))
    bits = [
        jnp.sum(jnp.where(lane8 // 16 == k, live8 * bit, 0), axis=1, keepdims=True) for k in range(2)
    ]
    lane1 = iota((1, 128), 1)
    message = jnp.zeros((1, 128), I32)
    for b in range(BLK):
        message = jnp.where(lane1 == b * 16, own[b], message)
        for k in range(2):
            message = jnp.where(lane1 == b * 16 + 1 + k, bits[k][b : b + 1, :], message)
    idm[...] = message
    def send_ids(m, t, to):
        rem(idm, idr.at[me], ids_s, ids_r, (to, j)).start()

    each_patch(send_ids)
    idr[me] = idm[...]

    rank8[...] = jnp.where(live8 > 0, dot(live8.astype(F32).astype(BF), low_tri), -1.0)
    wide_k = iota((1, BLK * RT), 1)
    owner_row = jnp.zeros((1, BLK * RT), I32)
    for b in range(BLK):
        owner_row = jnp.where(wide_k // RT == b, own[b], owner_row)
    rid = iota((PATCH * RT, BLK * RT), 0)
    putm[...] = hot((rid // RT == owner_row) & (lax.rem(rid, RT) == lax.rem(wide_k, RT)))

    phase("z2")
    z_to_d(2)
    phase("z5w")
    landed(wz[5])
    wd[5] = weights_d(5)
    phase("w_edges")
    landed(edges_in)
    landed(vecs)
    phase("w_d0")
    landed(wd[0])
    phase("edge1")
    for jr in range(4):
        acc[:, jr * FEAT : (jr + 1) * FEAT] = dot(xe[...], wa[jr, 0]) + vec[pairs[jr], 0:1, :]
    gain = [jnp.concatenate([vec[k, i : i + 1, :] for k in range(4)], axis=1) for i in (1, 2, 4, 5)]
    phase("z7")
    z_to_d(7)
    phase("n3")
    landed(wy[6])
    wz[6] = weights_round(6)
    wy_to_x(3)
    phase("w_rows0")
    landed(rows_in[0:3])
    phase("w_d")
    landed(wd[1])
    landed(wd[2])
    landed(wd[5])
    landed(wd[7])

    def norm(mixed, gain_row, shift_row):
        mean = jnp.sum(mixed, axis=1, keepdims=True) * (1.0 / WIDE)
        spread = jnp.sum(mixed * mixed, axis=1, keepdims=True) * (1.0 / WIDE) - mean * mean
        return (mixed - mean) * lax.rsqrt(spread + EPS) * gain_row + shift_row

    phase("section")
    section = [dot(xs[0 : 2 * HALO, :], wa[k, 2]).astype(BF) for k in range(4)]
    phase("w_rows1")
    both = jnp.concatenate([rcol[2 * j], rcol[2 * j + 1]], axis=0)
    lane2 = iota((ROWS, 2 * HALO), 1)
    base2 = (iota((ROWS, 2 * HALO), 0) // TILE) * HALO
    take = hot((both >= 0) & (both + base2 == lane2))
    landed(rows_in[3:6])
    for u in (4, 8):
        wy[u] = weights_y(u)
    phase("edge2a")
    for k in range(4):
        cols = slice(k * FEAT, (k + 1) * FEAT)
        pre = acc[:, cols] + dot(xs[2 * HALO :, :], wa[k, 1]) + dot(take, section[k])
        hid[:, cols] = silu(pre).astype(BF)
    phase("x346")
    phase("edge2b")
    first = jnp.zeros((ROWS, 1), F32)
    second = jnp.zeros((ROWS, 1), F32)
    for n in range(4):
        cols = slice(n * FEAT, (n + 1) * FEAT)
        mixed = None
        for k in range(4):
            term = dot(hid[:, k * FEAT : (k + 1) * FEAT], wb[k, 0, :, cols]).astype(BF).astype(F32)
            mixed = term if mixed is None else mixed + term
        acc[:, cols] = mixed
        first = first + jnp.sum(mixed, axis=1, keepdims=True)
        second = second + jnp.sum(mixed * mixed, axis=1, keepdims=True)
    mean = first * (1.0 / WIDE)
    scale = lax.rsqrt(second * (1.0 / WIDE) - mean * mean + EPS)
    member = []
    for bb in range(2):
        rank_row = rank8[pl.ds(2 * j + bb, 1), :][:, 0:HALO]
        which = hot(rank_row == iota((RT, HALO), 0).astype(F32))
        match = hot(rcv[pl.ds(2 * j + bb, 1), :] == iota((HALO, TILE), 0))
        member.append(dot(which, match).astype(BF))
    for n in range(4):
        cols = slice(n * FEAT, (n + 1) * FEAT)
        old = xe[:, cols].astype(F32)
        fresh = (acc[:, cols] - mean) * scale * gain[0][:, cols] + gain[1][:, cols]
        fresh = jnp.where(both >= 0, old + fresh, old).astype(BF)
        outb[:, cols] = fresh
        for bb in range(2):
            part = dot(member[bb], fresh[bb * TILE : (bb + 1) * TILE, :])
            tsb[bb * RT : (bb + 1) * RT, cols] = part.astype(BF)

    phase("esend")
    my_sums = pl.ds(aligned(j * 2 * RT, 2 * RT), 2 * RT)

    def cols_of(dy):
        return pl.ds(aligned(pairs[dy] * FEAT, FEAT), FEAT)

    sums = start([
        rem(
            tsb.at[:, cols_of(dy)], tsr.at[my_sums], tss.at[dy - 1], tsrr.at[dy - 1],
            (me, pairs[dy]),
        )
        for dy in (2, 1, 3)
    ])
    tsr[my_sums, :] = tsb[:, my_cols]
    phase("n36")
    x_to_z(3)
    phase("n48")
    wy_to_x(4)
    wy_to_x(8)
    nodes_in = start([
        rem(
            nl.at[pl.ds(aligned(pairs[dy] * NROW, NROW), NROW)], xn.at[:, my_cols],
            xns.at[dy - 1], xnr.at[dy - 1], (me, pairs[dy]),
        )
        for dy in (2, 1, 3)
    ])
    edges_out = start([
        rem(
            outb.at[:, cols_of(dy)], o_e.at[my_edges], oes.at[dy - 1], oer.at[dy - 1],
            (me, pairs[dy]),
        )
        for dy in (2, 1, 3)
    ])
    phase("w_sums")
    landed(sums)
    phase("sumsend")
    sv[...] = dot(putm[...], tsr[...]).astype(BF)
    my_slot = pl.ds(aligned(me * RT, RT), RT)

    def send_sum(m, t, to):
        rem(sv.at[pl.ds(aligned(to * RT, RT), RT)], vv.at[my_slot], v2s, v2r, (to, j)).start()

    each_patch(send_sum)
    vv[my_slot, :] = sv[my_slot, :]

    order = (2, 1, 3, 0)
    half_n = NROW // 2

    def tables():
        all_ids = pltpu.make_async_copy(idr.at[pl.ds(0, 63)], idr.at[pl.ds(0, 63)], ids_r)
        all_ids.wait()
        ids = idr[:, 0, :]
        bits = [jnp.zeros((PATCH, 1), I32) for _ in range(2)]
        for b in range(BLK):
            held = ids[:, b * 16 : b * 16 + 1] == me
            for k in range(2):
                bits[k] = jnp.where(held, ids[:, b * 16 + 1 + k : b * 16 + 2 + k], bits[k])
        lane2 = iota((PATCH, 128), 1)
        seen = jnp.where(lane2 < 16, bits[0], bits[1])
        seen = lax.shift_right_logical(seen + jnp.zeros_like(lane2), lax.rem(lane2, 16))
        seen = jnp.where(lane2 < HALO, lax.rem(seen, 2), 0)
        rank = jnp.where(seen > 0, dot(seen.astype(F32).astype(BF), low_tri), -1.0)
        listed = jnp.concatenate([hal[...], jnp.zeros((HALO, PATCH), I32)], axis=1)
        listed = jnp.concatenate([listed, jnp.zeros((128 - HALO, 128), I32)], axis=0)
        listed = listed.T[0:PATCH].astype(F32) + 1.0
        wide = iota((PATCH, PATCH * RT), 1)
        mine = wide // RT == iota((PATCH, PATCH * RT), 0)
        spread = jnp.zeros((PATCH, PATCH * RT), F32)
        for r in range(RT):
            node_r = jnp.sum(jnp.where(rank == float(r), listed, 0.0), axis=1, keepdims=True)
            spread = jnp.where(mine & (lax.rem(wide, RT) == r), node_r, spread)
        node_of = jnp.sum(spread, axis=0, keepdims=True).astype(I32) - 1
        for h in range(2):
            for i, dy in enumerate(order):
                low = (4 * h + i) * half_n
                node = iota((half_n, PATCH * RT), 0) + (pairs[dy] * NROW + h * half_n)
                amat[low : low + half_n, :] = hot(node == node_of)

    phase("w_ny")
    phase("eout")
    o_e[my_edges, :] = outb[:, my_cols]
    phase("w_n3")
    z_to_d(3)
    phase("w_n6")
    z_to_d(6)
    phase("w_ids")
    tables()
    phase("w_nx")
    x_to_z(4)
    x_to_z(8)
    phase("w_nin")
    landed(nodes_in)
    phase("w_nd")
    landed(wd[3])
    phase("node1")
    for jr in range(4):
        acc2[:, jr * FEAT : (jr + 1) * FEAT] = dot(xn[...], wa[jr, 3]) + vec[pairs[jr], 3:4, :]

    phase("w_vv")
    got = vv.at[pl.ds(0, 63 * RT)]
    pltpu.make_async_copy(got, got, v2r).wait()
    phase("agg")
    agg_in = []
    for h in range(2):
        rows = slice(h * half_n, (h + 1) * half_n)
        parts = dot(amat[4 * h * half_n : 4 * (h + 1) * half_n, :], vv[...]).astype(BF)
        for i, dy in enumerate(order):
            part = parts[i * half_n : (i + 1) * half_n, :]
            if dy == 0:
                xa[rows, my_cols] = part
            else:
                abuf[dy - 1, rows, :] = part
                agg_in.append(rem(
                    abuf.at[dy - 1, rows], xa.at[rows, my_cols], as_.at[h, dy - 1],
                    ar_.at[h, dy - 1], (me, pairs[dy]),
                ))
                start(agg_in[-1:])
    phase("w_nz")
    z_to_d(4)
    z_to_d(8)
    phase("w_nd2")
    for u in (6, 4, 8):
        landed(wd[u])
    nodes_out = []
    for h in range(2):
        phase("w_agg%d" % h)
        landed(agg_in[3 * h : 3 * h + 3])
        phase("node2_%d" % h)
        rows = slice(h * half_n, (h + 1) * half_n)
        mixed = None
        for jr in range(4):
            cols = slice(jr * FEAT, (jr + 1) * FEAT)
            hidden = silu(acc2[rows, cols] + dot(xa[rows, :], wa[jr, 4])).astype(BF)
            term = dot(hidden, wb[jr, 1]).astype(BF).astype(F32)
            mixed = term if mixed is None else mixed + term
        old = xn[rows, :].astype(F32)
        live = iota((half_n, 1), 0) + (j * NROW + h * half_n) < cnt[0]
        outn[rows, :] = jnp.where(live, old + norm(mixed, gain[2], gain[3]), old).astype(BF)
        to_rows = pl.ds(aligned(j * NROW + h * half_n, half_n), half_n)
        nodes_out.extend(start([
            rem(
                outn.at[rows, cols_of(dy)], o_n.at[to_rows], ons.at[h, dy - 1], onr.at[h, dy - 1],
                (me, pairs[dy]),
            )
            for dy in (2, 1, 3)
        ]))
        o_n[to_rows, :] = outn[rows, my_cols]

    phase("end_s")
    done = picked.at[pl.ds(0, 63 * HALO)]
    pltpu.make_async_copy(done, done, hs).wait()
    pltpu.make_async_copy(idr.at[pl.ds(0, 63)], idr.at[pl.ds(0, 63)], ids_s).wait()
    pltpu.make_async_copy(got, got, v2s).wait()
    for copy in sent:
        copy.wait_send()
    phase("end_e")
    landed(edges_out)
    phase("end_n")
    landed(nodes_out)
    phase(None)


def shards(
    node_latents, edge_latents, edge_sender, edge_receiver, block_owner, node_counts, halo_nodes,
    w_endpoints, w_edge_in, edge_bias, w_edge_out, edge_gain, edge_shift, w_node_in, node_bias,
    w_node_out, node_gain, node_shift,
):
    row = lambda v: v.reshape(1, FEAT)
    dma = pltpu.SemaphoreType.DMA
    vm = pltpu.VMEM
    scratch = [
        pltpu.SMEM((BLK,), I32), pltpu.SMEM((1,), I32), vm((BLK, TILE), I32), vm((BLK, TILE), I32), vm((HALO, PATCH), I32),
        vm((NODE, FEAT), BF), vm((EDGE, 1), I32), vm((EDGE, FEAT), BF), vm((EDGE, FEAT), BF),
        vm((4, SEL, 1), I32), vm((BLK, TILE, 1), I32), vm((BLK, 128), I32), vm((1, 128), I32),
        vm((BLK, 128), F32),
        vm((PATCH, 1, 128), I32), vm((4, 8, FEAT), F32), vm((4, SEL, FEAT), F32),
        vm((3, SEL, FEAT), BF), vm((SEL, WIDE), BF), vm((ROWS, WIDE), BF), vm((NROW, WIDE), BF),
        vm((4, 5, WIDE, FEAT), BF), vm((4, 2, FEAT, WIDE), BF), vm((WIDE, 2, FEAT), BF),
        vm((ROWS, WIDE), F32), vm((ROWS, WIDE), BF), vm((ROWS, WIDE), BF), vm((2 * RT, WIDE), BF),
        vm((BLK * RT, FEAT), BF), vm((PATCH * RT, FEAT), BF), vm((PATCH * RT, FEAT), BF),
        vm((NODE, PATCH * RT), BF), vm((PATCH * RT, BLK * RT), BF), vm((3, NROW, FEAT), BF),
        vm((NROW, WIDE), BF), vm((NROW, WIDE), F32), vm((NROW, WIDE), BF),
        dma((22,)), dma, dma((4,)), dma, dma, dma((3,)), dma((3,)), dma((3,)), dma((3,)),
        dma((3,)), dma((3,)), dma((9, 3)), dma((9, 3)), dma((9, 2)), dma((9, 2)), dma((9, 2)),
        dma((9, 2)), dma((2, 7)), dma((2, 7)), dma((9,)), dma((9,)), dma((2, 3)), dma((2, 3)), dma((3,)), dma((3,)), dma,
        dma, dma((2, 3)), dma((2, 3)), dma((3,)), dma((3,)), dma((2, 3)), dma((2, 3)),
    ]
    return pl.pallas_call(
        kernel,
        out_shape=(
            vm((NODE, FEAT), BF),
            vm((EDGE, FEAT), BF),
        ),
        in_specs=[ANY] * 18,
        out_specs=(VM, VM),
        scratch_shapes=scratch,
        compiler_params=pltpu.CompilerParams(
            collective_id=0, has_side_effects=True, vmem_limit_bytes=60 * 2**20
        ),
        name="layer",
    )(
        node_latents, edge_latents, edge_sender, edge_receiver, block_owner, node_counts,
        halo_nodes[0].T, w_endpoints, w_edge_in, row(edge_bias), w_edge_out,
        row(edge_gain), row(edge_shift), w_node_in, row(node_bias), w_node_out, row(node_gain),
        row(node_shift),
    )


def solution(mesh):
    return jax.shard_map(
        shards,
        mesh=mesh,
        in_specs=(
            P("patch", "pair"),
            P("patch", "pair"),
            P("patch", None),
            P("patch", None),
            P("patch"),
            P("patch"),
            P("patch", None, None),
            P(None, None, "pair"),
            P(None, "pair"),
            P("pair"),
            P("pair", None),
            P("pair"),
            P("pair"),
            P(None, None, "pair"),
            P("pair"),
            P("pair", None),
            P("pair"),
            P("pair"),
        ),
        out_specs=(P("patch", "pair"), P("patch", "pair")),
        check_vma=False,
    )
```
